16 devices in a mesh: dp: 4 (over z, y), sp: 4 (over x, core).
Axes of the slice: x: 2, y: 2, z: 2, core: 2. Of those that a mesh axis runs over, the one named last changes fastest.
Arguments:
- latents: bfloat16 [24, 8, 128, 1280], P('dp', 'sp'), parts along dimension 0
- time_emb: bfloat16 [24, 1280], P('dp'), parts along dimension 0
- context: bfloat16 [24, 77, 1024], P('dp'), parts along dimension 0
- res_norm: float32 [2, 2, 2, 1280], replicated
- res_conv_w: bfloat16 [2, 2, 3, 3, 1280, 1280], replicated
- res_conv_b: float32 [2, 2, 1280], replicated
- res_temb_w: bfloat16 [2, 1280, 1280], replicated
- res_temb_b: float32 [2, 1280], replicated
- tr_norm: float32 [2, 1280], replicated
- proj_w: bfloat16 [2, 1280, 1280], replicated
- proj_b: float32 [2, 1280], replicated
- ln_par: float32 [2, 3, 2, 1280], replicated
- self_qkv: bfloat16 [2, 3, 1280, 20, 64], replicated
- cross_q: bfloat16 [2, 1280, 20, 64], replicated
- cross_kv: bfloat16 [2, 2, 1024, 20, 64], replicated
- attn_out: bfloat16 [2, 2, 20, 64, 1280], replicated
- attn_b: float32 [2, 2, 1280], replicated
- ff_in_w: bfloat16 [2, 1280, 10240], replicated
- ff_in_b: float32 [2, 10240], replicated
- ff_out_w: bfloat16 [2, 5120, 1280], replicated
- ff_out_b: float32 [2, 1280], replicated
Outputs:
- output: bfloat16 [24, 8, 128, 1280], P('dp', 'sp'), parts along dimension 0
There are 4 independent parts. The reference program is written for one: setup_inputs(seed, part) draws one part's arguments, and reference() takes and returns one part's arrays. A program takes and returns all parts, laid end to end along the dimension named above; an argument that names none is the same for every part.
All inputs are finite; a program needn't handle non-finite values.
Results may differ from the reference program's by a relative error of at most 0.0194881.
Values are sent between devices in bfloat16 or wider.
A program may use at most 1.25 GiB of HBM per device.

```python
import math
import jax
import jax.numpy as jnp
from jax import lax

IMG_BATCH = 6
IMG_ROWS = 8
IMG_WIDTH = 128
CHANNELS = 1280
NUM_HEADS = 20
TIME_DIM = 1280
CTX_DIM = 1024
CTX_LEN = 77
NUM_GROUPS = 32
FF_DIM = 5120

NUM_TOKENS = IMG_ROWS * IMG_WIDTH
HEAD_DIM = CHANNELS // NUM_HEADS
ATTN_SCALE = 1.0 / math.sqrt(HEAD_DIM)


def scaled_normal(rng_key, arr_shape, fan_in):
    return jax.random.normal(rng_key, arr_shape, jnp.float32) / math.sqrt(fan_in)


def setup_inputs(seed: int = 0, part: int = 0) -> dict:
    part_keys = jax.random.split(jax.random.fold_in(jax.random.key(seed + 1), part), 6)
    wt_keys = jax.random.split(jax.random.key(seed), 18)
    row_pos = jnp.arange(IMG_ROWS, dtype=jnp.float32)[None, :, None, None] * (math.pi / IMG_ROWS)
    mean_phase = jnp.repeat(jax.random.uniform(part_keys[0], (IMG_BATCH, 1, 1, NUM_GROUPS), jnp.float32, 0.0, 2.0 * math.pi), CHANNELS // NUM_GROUPS, axis=-1)
    scale_phase = jax.random.uniform(part_keys[1], (IMG_BATCH, 1, 1, CHANNELS), jnp.float32, 0.0, 2.0 * math.pi)
    chan_shift = 0.3 * jax.random.normal(part_keys[2], (IMG_BATCH, 1, 1, CHANNELS), jnp.float32)
    noise_val = jax.random.normal(part_keys[3], (IMG_BATCH, IMG_ROWS, IMG_WIDTH, CHANNELS), jnp.float32)
    latents = noise_val * (1.0 + 0.5 * jnp.cos(row_pos + scale_phase)) + 0.8 * jnp.sin(row_pos + mean_phase) + chan_shift
    time_emb = jax.random.normal(part_keys[4], (IMG_BATCH, TIME_DIM), jnp.float32)
    context = jax.random.normal(part_keys[5], (IMG_BATCH, CTX_LEN, CTX_DIM), jnp.float32)
    sharp_self = 0.8 * math.sqrt(math.log(NUM_TOKENS))
    sharp_cross = 0.8 * math.sqrt(math.log(CTX_LEN))
    affine_base = jnp.array([1.0, 0.0], jnp.float32)[:, None]
    qkv_gain = jnp.array([sharp_self, 1.0, 2.0], jnp.float32)[:, None, None, None]
    kv_gain = jnp.array([1.0, 2.0], jnp.float32)[:, None, None, None]
    return {
        'latents': latents.astype(jnp.bfloat16),
        'time_emb': time_emb.astype(jnp.bfloat16),
        'context': context.astype(jnp.bfloat16),
        'res_norm': affine_base + 0.25 * jax.random.normal(wt_keys[0], (2, 2, 2, CHANNELS), jnp.float32),
        'res_conv_w': scaled_normal(wt_keys[1], (2, 2, 3, 3, CHANNELS, CHANNELS), 9 * CHANNELS).astype(jnp.bfloat16),
        'res_conv_b': 0.3 * jax.random.normal(wt_keys[2], (2, 2, CHANNELS), jnp.float32),
        'res_temb_w': scaled_normal(wt_keys[3], (2, TIME_DIM, CHANNELS), TIME_DIM).astype(jnp.bfloat16),
        'res_temb_b': 0.3 * jax.random.normal(wt_keys[4], (2, CHANNELS), jnp.float32),
        'tr_norm': affine_base + 0.25 * jax.random.normal(wt_keys[5], (2, CHANNELS), jnp.float32),
        'proj_w': scaled_normal(wt_keys[6], (2, CHANNELS, CHANNELS), CHANNELS).astype(jnp.bfloat16),
        'proj_b': 0.3 * jax.random.normal(wt_keys[7], (2, CHANNELS), jnp.float32),
        'ln_par': affine_base + 0.25 * jax.random.normal(wt_keys[8], (2, 3, 2, CHANNELS), jnp.float32),
        'self_qkv': (scaled_normal(wt_keys[9], (2, 3, CHANNELS, NUM_HEADS, HEAD_DIM), CHANNELS) * qkv_gain).astype(jnp.bfloat16),
        'cross_q': (scaled_normal(wt_keys[10], (2, CHANNELS, NUM_HEADS, HEAD_DIM), CHANNELS) * sharp_cross).astype(jnp.bfloat16),
        'cross_kv': (scaled_normal(wt_keys[11], (2, 2, CTX_DIM, NUM_HEADS, HEAD_DIM), CTX_DIM) * kv_gain).astype(jnp.bfloat16),
        'attn_out': scaled_normal(wt_keys[12], (2, 2, NUM_HEADS, HEAD_DIM, CHANNELS), CHANNELS).astype(jnp.bfloat16),
        'attn_b': 0.3 * jax.random.normal(wt_keys[13], (2, 2, CHANNELS), jnp.float32),
        'ff_in_w': scaled_normal(wt_keys[14], (2, CHANNELS, 2 * FF_DIM), CHANNELS).astype(jnp.bfloat16),
        'ff_in_b': 0.3 * jax.random.normal(wt_keys[15], (2, 2 * FF_DIM), jnp.float32),
        'ff_out_w': scaled_normal(wt_keys[16], (2, FF_DIM, CHANNELS), FF_DIM).astype(jnp.bfloat16),
        'ff_out_b': 0.3 * jax.random.normal(wt_keys[17], (2, CHANNELS), jnp.float32),
    }


def matmul_f32(form, left, right):
    return jnp.einsum(form, left.astype(jnp.float32), right.astype(jnp.float32))


def group_norm(values, norm_gain, norm_bias, eps_val):
    grouped = values.astype(jnp.float32).reshape(IMG_BATCH, IMG_ROWS, IMG_WIDTH, NUM_GROUPS, CHANNELS // NUM_GROUPS)
    grp_mean = grouped.mean(axis=(1, 2, 4), keepdims=True)
    grp_sq = (grouped * grouped).mean(axis=(1, 2, 4), keepdims=True)
    normed = (grouped - grp_mean) * lax.rsqrt(grp_sq - grp_mean * grp_mean + eps_val)
    return normed.reshape(IMG_BATCH, IMG_ROWS, IMG_WIDTH, CHANNELS) * norm_gain + norm_bias


def conv_same(act_in, kernel):
    return lax.conv_general_dilated(act_in.astype(jnp.float32), kernel.astype(jnp.float32), (1, 1), 'SAME', dimension_numbers=('NHWC', 'HWIO', 'NHWC'))


def resnet(latents, time_emb, res_index, res_norm, res_conv_w, res_conv_b, res_temb_w, res_temb_b):
    first_act = jax.nn.silu(group_norm(latents, res_norm[res_index, 0, 0], res_norm[res_index, 0, 1], 1e-5)).astype(jnp.bfloat16)
    time_proj = jnp.dot(jax.nn.silu(time_emb.astype(jnp.float32)).astype(jnp.bfloat16), res_temb_w[res_index], preferred_element_type=jnp.float32) + res_temb_b[res_index]
    hidden = (conv_same(first_act, res_conv_w[res_index, 0]) + res_conv_b[res_index, 0] + time_proj[:, None, None, :]).astype(jnp.bfloat16)
    second_act = jax.nn.silu(group_norm(hidden, res_norm[res_index, 1, 0], res_norm[res_index, 1, 1], 1e-5)).astype(jnp.bfloat16)
    update = conv_same(second_act, res_conv_w[res_index, 1]) + res_conv_b[res_index, 1]
    return (latents.astype(jnp.float32) + update).astype(jnp.bfloat16)


def layer_norm(values, norm_gain, norm_bias):
    centered = values.astype(jnp.float32)
    centered = centered - centered.mean(axis=-1, keepdims=True)
    variance = (centered * centered).mean(axis=-1, keepdims=True)
    return (centered * lax.rsqrt(variance + 1e-5) * norm_gain + norm_bias).astype(jnp.bfloat16)


def attend_block(q_blk, k_all, v_all):
    scores = matmul_f32('bqhd,bkhd->bhqk', q_blk, k_all) * ATTN_SCALE
    row_exp = jnp.exp(scores - scores.max(axis=-1, keepdims=True))
    row_sum = row_exp.sum(axis=-1)
    row_out = matmul_f32('bhqk,bkhd->bqhd', row_exp.astype(jnp.bfloat16), v_all)
    return (row_out / jnp.swapaxes(row_sum, 1, 2)[..., None]).astype(jnp.bfloat16)


def transformer(hidden, context, tr_norm, proj_w, proj_b, ln_par, self_qkv, cross_q, cross_kv, attn_out, attn_b, ff_in_w, ff_in_b, ff_out_w, ff_out_b):
    normed = group_norm(hidden, tr_norm[0], tr_norm[1], 1e-6).astype(jnp.bfloat16).reshape(IMG_BATCH, NUM_TOKENS, CHANNELS)
    hidden_tok = (matmul_f32('bnc,cd->bnd', normed, proj_w[0]) + proj_b[0]).astype(jnp.bfloat16)

    def block_fn(carried, layer_w):
        ln_w, qkv_w, cq_w, ckv_w, out_w, out_b, ffi_w, ffi_b, ffo_w, ffo_b = layer_w
        normed_one = layer_norm(carried, ln_w[0, 0], ln_w[0, 1])
        q_all = matmul_f32('bnc,chd->bnhd', normed_one, qkv_w[0]).astype(jnp.bfloat16)
        k_all = matmul_f32('bnc,chd->bnhd', normed_one, qkv_w[1]).astype(jnp.bfloat16)
        v_all = matmul_f32('bnc,chd->bnhd', normed_one, qkv_w[2]).astype(jnp.bfloat16)
        q_rows = jnp.swapaxes(q_all.reshape(IMG_BATCH, IMG_ROWS, IMG_WIDTH, NUM_HEADS, HEAD_DIM), 0, 1)
        attended = lax.map(lambda q_row: attend_block(q_row, k_all, v_all), q_rows)
        attended = jnp.swapaxes(attended, 0, 1).reshape(IMG_BATCH, NUM_TOKENS, NUM_HEADS, HEAD_DIM)
        carried = (carried.astype(jnp.float32) + matmul_f32('bnhd,hdc->bnc', attended, out_w[0]) + out_b[0]).astype(jnp.bfloat16)
        normed_two = layer_norm(carried, ln_w[1, 0], ln_w[1, 1])
        q_cross = matmul_f32('bnc,chd->bnhd', normed_two, cq_w).astype(jnp.bfloat16)
        k_cross = matmul_f32('btc,chd->bthd', context, ckv_w[0]).astype(jnp.bfloat16)
        v_cross = matmul_f32('btc,chd->bthd', context, ckv_w[1]).astype(jnp.bfloat16)
        crossed = attend_block(q_cross, k_cross, v_cross)
        carried = (carried.astype(jnp.float32) + matmul_f32('bnhd,hdc->bnc', crossed, out_w[1]) + out_b[1]).astype(jnp.bfloat16)
        normed_three = layer_norm(carried, ln_w[2, 0], ln_w[2, 1])
        ff_proj = matmul_f32('bnc,cf->bnf', normed_three, ffi_w) + ffi_b
        gated_act = (ff_proj[..., :FF_DIM] * jax.nn.gelu(ff_proj[..., FF_DIM:], approximate=False)).astype(jnp.bfloat16)
        carried = (carried.astype(jnp.float32) + matmul_f32('bnf,fc->bnc', gated_act, ffo_w) + ffo_b).astype(jnp.bfloat16)
        return carried, None

    hidden_tok, _unused = lax.scan(block_fn, hidden_tok, (ln_par, self_qkv, cross_q, cross_kv, attn_out, attn_b, ff_in_w, ff_in_b, ff_out_w, ff_out_b))
    out_tok = matmul_f32('bnc,cd->bnd', hidden_tok, proj_w[1]) + proj_b[1] + hidden.reshape(IMG_BATCH, NUM_TOKENS, CHANNELS).astype(jnp.float32)
    return out_tok.astype(jnp.bfloat16).reshape(IMG_BATCH, IMG_ROWS, IMG_WIDTH, CHANNELS)


def reference(latents, time_emb, context, res_norm, res_conv_w, res_conv_b, res_temb_w, res_temb_b, tr_norm, proj_w, proj_b, ln_par, self_qkv, cross_q, cross_kv, attn_out, attn_b, ff_in_w, ff_in_b, ff_out_w, ff_out_b):
    first_out = resnet(latents, time_emb, 0, res_norm, res_conv_w, res_conv_b, res_temb_w, res_temb_b)
    middle = transformer(first_out, context, tr_norm, proj_w, proj_b, ln_par, self_qkv, cross_q, cross_kv, attn_out, attn_b, ff_in_w, ff_in_b, ff_out_w, ff_out_b)
    return resnet(middle, time_emb, 1, res_norm, res_conv_w, res_conv_b, res_temb_w, res_temb_b)
```

```python
import functools
import math
import jax
import jax.numpy as jnp
from jax import lax
from jax.experimental import pallas as pl
from jax.experimental.pallas import tpu as pltpu
from jax.sharding import PartitionSpec as P

F32 = jnp.float32
BF = jnp.bfloat16
HIGHEST = lax.Precision.HIGHEST
NT = (((1,), (1,)), ((), ()))
NUM_GROUPS = 32
HEAD = 64
LANES = 128
MIB = 2 ** 20
LATENTS = 3
KERNEL = 3
WIDE = 256
SUM_ROWS = 8
CTX_ROWS = 80
SOFTMAX_MUL = math.log2(math.e) / math.sqrt(HEAD)

def params(mib):
    return pltpu.CompilerParams(vmem_limit_bytes=mib * MIB)


def cost(flops, nbytes):
    return pl.CostEstimate(flops=int(flops), bytes_accessed=int(nbytes), transcendentals=0)


def fixed(shape, *lead):
    index = tuple(lead) + (0,) * (len(shape) - len(lead))
    return pl.BlockSpec(tuple(shape), lambda *_: index, pipeline_mode=pl.Buffered(1))


def whole(array):
    return fixed(array.shape)


def major(shape):
    return pl.BlockSpec(tuple(shape), lambda b, *_: (b,) + (0,) * (len(shape) - 1))


def minor(shape, lead=0):
    return pl.BlockSpec(tuple(shape), lambda n, *_: (lead,) + (0,) * (len(shape) - 2) + (n,))


def any_space():
    return pl.BlockSpec(memory_space=pl.ANY)


def dot(left, right):
    return jnp.dot(left, right, preferred_element_type=F32)


def dot_nt(left, right):
    return lax.dot_general(left, right, NT, preferred_element_type=F32)


def col_sum(values):
    return jnp.sum(values, axis=0, keepdims=True)


def col_max(values):
    return jnp.max(values, axis=0, keepdims=True)


def row_of(ref, *index):
    return ref[index][None, :]


def affine(ref, *index):
    return row_of(ref, *index, 0), row_of(ref, *index, 1)


def like(array, dtype=BF):
    return jax.ShapeDtypeStruct(tuple(array), dtype)


def at_lanes(index, size=LANES):
    return slice(index * size, (index + 1) * size)


def pairs_of(text):
    return [tuple(map(int, pair)) for pair in text.split()]


def group_stats(totals, lat, count, eps):
    chan = totals.shape[1]
    per = chan // NUM_GROUPS
    fold = (lax.broadcasted_iota(jnp.int32, (chan, LANES), 0) // per == lax.broadcasted_iota(jnp.int32, (chan, LANES), 1)).astype(F32)
    spread = (lax.broadcasted_iota(jnp.int32, (LANES, chan), 1) // per == lax.broadcasted_iota(jnp.int32, (LANES, chan), 0)).astype(F32)
    grouped = jnp.dot(totals, fold, precision=HIGHEST, preferred_element_type=F32) * (1.0 / (count * per))
    means = jnp.dot(grouped, spread, precision=HIGHEST, preferred_element_type=F32)
    mean = means[0:lat]
    return mean, lax.rsqrt(means[lat:2 * lat] - mean * mean + eps)


def layer_norm(values, gain, bias):
    centered = values - jnp.mean(values, axis=-1, keepdims=True)
    variance = jnp.mean(centered * centered, axis=-1, keepdims=True)
    return (centered * lax.rsqrt(variance + 1e-5) * gain + bias).astype(BF)


def place_rows(sums, squares, base):
    zero = jnp.zeros_like(sums[0])
    rows = [zero] * SUM_ROWS
    for l, (one, two) in enumerate(zip(sums, squares)):
        rows[base + l] = one
        rows[LATENTS + base + l] = two
    return jnp.concatenate(rows, axis=0)


def conv_kernel(core_ref, v_ref, halo_ref, own_ref, peer_ref, norm_ref, bias_ref, *rest, res_i, conv_i, eps, base, has_temb, has_res, has_into, want_sums):
    rest = list(rest)
    temb_ref = rest.pop(0) if has_temb else None
    w_hbm = rest.pop(0)
    res_ref = rest.pop(0) if has_res else None
    acat, w_buf, w_sem = rest[-3:]
    rest = rest[:-3]
    before_ref = None
    if has_into:
        _, _, before_ref = rest[:3]
        rest = rest[3:]
    out_ref = rest.pop(0)
    sum_ref, edge_ref = rest if want_sums else (None, None)
    lat, tok, chan = v_ref.shape
    rows = tok // LANES
    core = core_ref[0]
    step, steps = pl.program_id(0), pl.num_programs(0)
    nt = out_ref.shape[-1]

    def fetch(n):
        lanes = pl.ds(pl.multiple_of(n * nt, LANES), nt)
        return pltpu.make_async_copy(w_hbm.at[2 * res_i + conv_i, :, :, lanes], w_buf.at[n % 2], w_sem.at[n % 2])

    @pl.when(step == 0)
    def _():
        fetch(0).start()
        fetch(1).start()
        mean, inv = group_stats(own_ref[...] + peer_ref[...], LATENTS, 2 * tok, eps)
        gain, shift = affine(norm_ref, res_i, conv_i)
        scale = inv * gain

        def emit(src, l, row, cs):
            g = base + l
            x = (src.astype(F32) - row_of(mean, g, cs)) * row_of(scale, g, cs) + shift[:, cs]
            half = 0.5 * x
            y = half * jnp.tanh(half) + half
            col = lax.broadcasted_iota(jnp.int32, y.shape, 0)
            left = jnp.where(col == 0, 0.0, pltpu.roll(y, 1, 0))
            right = jnp.where(col == LANES - 1, 0.0, pltpu.roll(y, LANES - 1, 0))
            rr = pl.ds(pl.multiple_of(row * LANES, LANES), LANES)
            for d, val in enumerate((left, y, right)):
                acat[l, rr, d * chan + cs.start:d * chan + cs.stop] = val.astype(BF)

        for l in range(lat):
            def one_row(r, carry):
                for ch in range(chan // WIDE):
                    cs = at_lanes(ch, WIDE)
                    emit(v_ref[l, pl.ds(pl.multiple_of(r * LANES, LANES), LANES), cs], l, r + 1, cs)
                return carry

            lax.fori_loop(0, rows, one_row, 0)
            for ch in range(chan // WIDE):
                cs = at_lanes(ch, WIDE)
                emit(halo_ref[l, :, cs], l, jnp.where(core == 0, rows + 1, 0), cs)
            rr = pl.ds(pl.multiple_of(jnp.where(core == 0, 0, rows + 1) * LANES, LANES), LANES)
            acat[l, rr, :] = jnp.zeros((LANES, KERNEL * chan), BF)

    slot = step % 2
    fetch(step).wait()
    sums, squares = [], []
    for l in range(lat):
        acc = row_of(bias_ref, res_i, conv_i)
        for dy in range(KERNEL):
            acc += dot(acat[l, dy * LANES:tok + dy * LANES, :], w_buf[slot, dy])
        if has_temb:
            acc += row_of(temb_ref, base + l)
        if has_res:
            acc += res_ref[l].astype(F32)
        out = acc.astype(BF)
        out_ref[l] = out
        if want_sums:
            edge_ref[l] = jnp.where(core == 0, out[tok - LANES:], out[:LANES])
            out = out.astype(F32)
            sums.append(col_sum(out))
            squares.append(col_sum(out * out))
    if want_sums:
        placed = place_rows(sums, squares, base)
        sum_ref[...] = placed + before_ref[...] if has_into else placed

    @pl.when(step + 2 < steps)
    def _():
        fetch(step + 2).start()


def conv_call(core, v, halo, own, peer, norm, bias, weights, res_i, conv_i, temb=None, res=None, into=None, base=0, lat=LATENTS, want_sums=True, nt=256):
    tok, chan = v.shape[1:]
    pick = lambda a: (base // lat if a.shape[0] > lat else 0)
    rows = lambda a: fixed((lat,) + a.shape[1:], pick(a))
    tile = lambda a, size: minor((lat, size, nt), pick(a))
    specs = [rows(v), rows(halo), whole(own), whole(peer), whole(norm), minor(bias.shape[:-1] + (nt,))]
    args = [v, halo, own, peer, norm, bias]
    if temb is not None:
        specs.append(minor((LATENTS, nt)))
        args.append(temb)
    specs.append(any_space())
    args.append(weights)
    if res is not None:
        specs.append(tile(res, tok))
        args.append(res)
    aliases = {}
    held = LATENTS if want_sums else lat
    out = like((held, tok, chan))
    if into is not None:
        aliases = {len(args) + 1: 0, len(args) + 2: 2}
        specs += [any_space(), any_space(), minor((SUM_ROWS, nt))]
        args += [into[0], into[2], into[1]]
    out_specs, out_shape = [tile(out, tok)], [out]
    if want_sums:
        out_specs += [minor((SUM_ROWS, nt)), tile(out, LANES)]
        out_shape += [like((SUM_ROWS, chan), F32), like((held, LANES, chan))]
    body = functools.partial(conv_kernel, res_i=res_i, conv_i=conv_i, eps=1e-5, base=base, has_temb=temb is not None, has_res=res is not None, has_into=into is not None, want_sums=want_sums)
    outs = pl.pallas_call(
        body,
        grid_spec=pltpu.PrefetchScalarGridSpec(
            num_scalar_prefetch=1, grid=(chan // nt,), in_specs=specs, out_specs=out_specs,
            scratch_shapes=[pltpu.VMEM((lat, tok + 2 * LANES, KERNEL * chan), BF), pltpu.VMEM((2, KERNEL, KERNEL * chan, nt), BF), pltpu.SemaphoreType.DMA((2,))]),
        out_shape=out_shape, compiler_params=params(60), input_output_aliases=aliases,
        cost_estimate=cost(18 * lat * tok * chan * chan, 18 * chan * chan), name="conv")(core, *args)
    return outs if want_sums else outs[0]


def gather_kernel(where_ref, own_ref, *rest, base, lat, has_into):
    firsts, seconds = rest[:lat], rest[lat:2 * lat]
    v_ref, sum_ref, edge_ref = rest[2 * lat + has_into:]
    index = where_ref[0]
    chip, core = index // 2, index % 2
    half = own_ref.shape[1]
    mine = jnp.logical_or(index == 0, index == 3)
    sums, squares = [], []
    for l in range(lat):
        third = jnp.where(mine, own_ref[l], seconds[l][0])
        first = firsts[l][0]
        top = jnp.where(chip == 0, third, first)
        bottom = jnp.where(chip == 0, first, third)
        v_ref[l, 0:half] = top
        v_ref[l, half:] = bottom
        edge_ref[l] = jnp.where(core == 0, bottom[half - LANES:], top[:LANES])
        top, bottom = top.astype(F32), bottom.astype(F32)
        sums.append(col_sum(top) + col_sum(bottom))
        squares.append(col_sum(top * top) + col_sum(bottom * bottom))
    sum_ref[...] = place_rows(sums, squares, base)


def gather_call(where, flat, firsts, seconds, base, into=None):
    lat = len(firsts)
    half, chan = flat.shape[1:]
    nt = 640
    part = minor((1, half, nt))
    specs = [pl.BlockSpec((pl.Element(lat), pl.Element(half), pl.Element(nt)), lambda n, w: (w[0] // 2 * LATENTS + base, 0, n * nt))] + [part] * (2 * lat)
    args = [flat, *firsts, *seconds]
    aliases = {}
    if into is not None:
        specs.append(any_space())
        args.append(into)
        aliases = {len(args): 0}
    return pl.pallas_call(
        functools.partial(gather_kernel, base=base, lat=lat, has_into=into is not None),
        grid_spec=pltpu.PrefetchScalarGridSpec(
            num_scalar_prefetch=1, grid=(chan // nt,), in_specs=specs,
            out_specs=[minor((lat, 2 * half, nt), base // lat), minor((SUM_ROWS, nt)), minor((lat, LANES, nt))]),
        out_shape=[like((LATENTS, 2 * half, chan)), like((SUM_ROWS, chan), F32), like((lat, LANES, chan))],
        input_output_aliases=aliases, compiler_params=params(60), cost_estimate=cost(MIB, 8 * lat * half * chan), name="gather")(where, *args)


def enter_kernel(h_ref, own_ref, peer_ref, norm_ref, pw_ref, pb_ref, ln_ref, wk_ref, u_ref, n_ref, k_ref, mean_s, scale_s):
    step = pl.program_id(0)
    lat = pl.num_programs(0)

    @pl.when(step == 0)
    def _():
        mean, inv = group_stats(own_ref[...] + peer_ref[...], LATENTS, 2 * h_ref.shape[1], 1e-6)
        mean_s[:LATENTS] = mean
        scale_s[:LATENTS] = inv * row_of(norm_ref, 0)

    mean, scale = mean_s[pl.ds(step, 1), :], scale_s[pl.ds(step, 1), :]
    normed = ((h_ref[0].astype(F32) - mean) * scale + row_of(norm_ref, 1)).astype(BF)
    u = (dot(normed, pw_ref[0]) + row_of(pb_ref, 0)).astype(BF)
    u_ref[0] = u
    n = layer_norm(u.astype(F32), *affine(ln_ref, 0, 0))
    n_ref[0] = n
    k_ref[0] = dot_nt(n, wk_ref[0, 0]).astype(BF)


def enter_call(h, own, peer, tr_norm, proj_w, proj_b, ln_par, qkv_t):
    lat, tok, chan = h.shape
    row = major((1, tok, chan))
    return pl.pallas_call(
        enter_kernel, grid=(lat,),
        in_specs=[row, whole(own), whole(peer), whole(tr_norm), fixed((1, chan, chan)), whole(proj_b), whole(ln_par), fixed((1, 1, chan, chan), 0, 1)],
        out_specs=[row] * 3, out_shape=[like(h.shape)] * 3,
        scratch_shapes=[pltpu.VMEM((SUM_ROWS, chan), F32)] * 2,
        compiler_params=params(60), cost_estimate=cost(4 * lat * tok * chan * chan, 4 * chan * chan), name="enter")(
            h, own, peer, tr_norm, proj_w, proj_b, ln_par, qkv_t)


def key_kernel(u_ref, ln_ref, wk_ref, n_ref, k_ref, *, layer):
    n = layer_norm(u_ref[0].astype(F32), *affine(ln_ref, layer, 0))
    n_ref[0] = n
    k_ref[0] = dot_nt(n, wk_ref[0, 0]).astype(BF)


def key_call(u, ln_par, qkv_t, layer):
    lat, tok, chan = u.shape
    row = major((1, tok, chan))
    return pl.pallas_call(
        functools.partial(key_kernel, layer=layer), grid=(lat,),
        in_specs=[row, whole(ln_par), fixed((1, 1, chan, chan), layer, 1)],
        out_specs=[row] * 2, out_shape=[like(u.shape)] * 2,
        compiler_params=params(60), cost_estimate=cost(2 * lat * tok * chan * chan, 2 * chan * chan), name="keys")(u, ln_par, qkv_t)


def query_kernel(n_ref, w_ref, q_ref):
    q_ref[0] = dot_nt(n_ref[0], w_ref[0, 0]).astype(BF)


def value_kernel(n_ref, w_ref, v_ref):
    v_ref[0] = dot_nt(w_ref[0, 0], n_ref[0]).astype(BF)


def linear_call(kernel, n, qkv_t, layer, part, out_block, name):
    lat, tok, chan = n.shape
    return pl.pallas_call(
        kernel, grid=(lat,),
        in_specs=[major((1, tok, chan)), fixed((1, 1, chan, chan), layer, part)],
        out_specs=major((1,) + out_block), out_shape=like((lat,) + out_block),
        compiler_params=params(60), cost_estimate=cost(tok * chan * chan // 4, 2 * chan * chan), name=name)(n, qkv_t)


def attn_kernel(q_ref, k0_ref, k1_ref, v0_ref, v1_ref, o_ref, *, pairs):
    def scores(i):
        p, h = divmod(i, 2)
        ls = slice(p * LANES, (p + 1) * LANES)
        q = q_ref[0, :, ls]
        lane = lax.broadcasted_iota(jnp.int32, q.shape, 1)
        qh = jnp.where((lane >= HEAD) == (h == 1), q, jnp.zeros_like(q))
        return [dot_nt(k_ref[0, :, ls], qh) for k_ref in (k0_ref, k1_ref)]

    coming = scores(0)
    halves = []
    for i in range(2 * pairs):
        s0, s1 = coming
        if i + 1 < 2 * pairs:
            coming = scores(i + 1)
        top = jnp.maximum(col_max(s0), col_max(s1))
        vs = slice(i * HEAD, (i + 1) * HEAD)
        e0 = jnp.exp2((s0 - top) * SOFTMAX_MUL)
        o = jnp.dot(v0_ref[0, vs, :], e0.astype(BF), preferred_element_type=F32)
        total = col_sum(e0)
        e1 = jnp.exp2((s1 - top) * SOFTMAX_MUL)
        o += jnp.dot(v1_ref[0, vs, :], e1.astype(BF), preferred_element_type=F32)
        total += col_sum(e1)
        halves.append(o / total)
        if i % 2:
            p = i // 2
            o_ref[0, :, p * LANES:(p + 1) * LANES] = jnp.transpose(jnp.concatenate(halves, axis=0)).astype(BF)
            halves = []


def attn_call(q, k0, k1, v0, v1, pairs=5):
    lat, tok, chan = q.shape
    width = LANES * pairs
    qs = pl.BlockSpec((1, tok, width), lambda b, h: (b, 0, h))
    vs = pl.BlockSpec((1, width, tok), lambda b, h: (b, h, 0))
    return pl.pallas_call(
        functools.partial(attn_kernel, pairs=pairs), grid=(lat, chan // width), in_specs=[qs, qs, qs, vs, vs], out_specs=qs,
        out_shape=like(q.shape), compiler_params=params(60),
        cost_estimate=cost(8 * lat * tok * tok * chan, 12 * lat * tok * chan), name="attn")(q, k0, k1, v0, v1)


def context_kernel(ctx_ref, w_ref, k_ref, v_ref):
    for l in range(ctx_ref.shape[0]):
        k_ref[0, l] = dot_nt(ctx_ref[l, 0:CTX_ROWS, :], w_ref[0, 0]).astype(BF)
        v_ref[0, l] = dot_nt(w_ref[0, 1], ctx_ref[l]).astype(BF)


def context_call(ctx, ckv_t):
    lat, padded, depth = ctx.shape
    layers, _, chan, _ = ckv_t.shape
    return pl.pallas_call(
        context_kernel, grid=(layers,),
        in_specs=[whole(ctx), major((1, 2, chan, depth))],
        out_specs=[major((1, lat, CTX_ROWS, chan)), major((1, lat, chan, padded))],
        out_shape=[like((layers, lat, CTX_ROWS, chan)), like((layers, lat, chan, padded))],
        compiler_params=params(60), cost_estimate=cost(4 * layers * lat * padded * depth * chan, 4 * layers * depth * chan), name="context")(ctx, ckv_t)


def post_kernel(att_ref, u_ref, wo_ref, ab_ref, ln_ref, wq_ref, kc_ref, vc_ref, wc_ref, out_ref, q_s, o_s, *, layer, ctx_len):
    tok, chan = u_ref.shape[1:]
    u = dot(att_ref[0], wo_ref[0, 0]) + u_ref[0].astype(F32) + row_of(ab_ref, layer, 0)
    u = u.astype(BF)
    out_ref[0] = u
    n = layer_norm(u.astype(F32), *affine(ln_ref, layer, 1))
    q_s[...] = dot_nt(n, wq_ref[0]).astype(BF)
    def scores(p):
        ls = at_lanes(p)
        kc = kc_ref[0, 0, :, ls]
        lane = lax.broadcasted_iota(jnp.int32, kc.shape, 1)
        zero = jnp.zeros_like(kc)
        both = jnp.concatenate([jnp.where(lane < HEAD, kc, zero), jnp.where(lane >= HEAD, kc, zero)], axis=0)
        return dot_nt(both, q_s[:, ls])

    pairs = chan // LANES
    coming = scores(0)
    for p in range(pairs):
        s = coming
        if p + 1 < pairs:
            coming = scores(p + 1)
        exps, sums = [], []
        for h in range(2):
            sh = s[at_lanes(h, CTX_ROWS)]
            valid = lax.broadcasted_iota(jnp.int32, sh.shape, 0) < ctx_len
            sh = jnp.where(valid, sh, -jnp.inf)
            e = jnp.exp2((sh - col_max(sh)) * SOFTMAX_MUL)
            sums.append(col_sum(e))
            exps += [e.astype(BF), jnp.zeros((LANES - CTX_ROWS, tok), BF)]
        vc = vc_ref[0, 0, at_lanes(p), :]
        row = lax.broadcasted_iota(jnp.int32, vc.shape, 0)
        zero = jnp.zeros_like(vc)
        vb = jnp.concatenate([jnp.where(row < HEAD, vc, zero), jnp.where(row >= HEAD, vc, zero)], axis=1)
        o = dot(vb, jnp.concatenate(exps, axis=0))
        o = jnp.concatenate([o[:HEAD] / sums[0], o[HEAD:] / sums[1]], axis=0)
        o_s[:, at_lanes(p)] = jnp.transpose(o).astype(BF)
    y = dot(o_s[...], wc_ref[0, 0]) + out_ref[0].astype(F32) + row_of(ab_ref, layer, 1)
    out_ref[0] = y.astype(BF)


def post_call(att, u, attn_out, attn_b, ln_par, cq_t, kc, vc, layer, ctx_len):
    lat, tok, chan = u.shape
    row = major((1, tok, chan))
    mat = lambda i: fixed((1, 1, chan, chan), layer, i)
    ctx_spec = lambda a: pl.BlockSpec((1, 1) + a.shape[2:], lambda b: (layer, b, 0, 0))
    return pl.pallas_call(
        functools.partial(post_kernel, layer=layer, ctx_len=ctx_len), grid=(lat,),
        in_specs=[row, row, mat(0), whole(attn_b), whole(ln_par), fixed((1, chan, chan), layer), ctx_spec(kc), ctx_spec(vc), mat(1)],
        out_specs=row, out_shape=like(u.shape),
        scratch_shapes=[pltpu.VMEM((tok, chan), BF)] * 2,
        compiler_params=params(60), cost_estimate=cost(6 * lat * tok * chan * chan, 6 * chan * chan), name="post")(
            att, u, attn_out, attn_b, ln_par, cq_t, kc, vc, attn_out)


def ffn_kernel(u_ref, ln_ref, w1a_ref, w1b_ref, b1a_ref, b1b_ref, w2_ref, b2_ref, out_ref, n_s, acc_s, *, layer, chunk):
    step = pl.program_id(0)
    tokens = u_ref.shape[0]

    @pl.when(step == 0)
    def _():
        def body(r, carry):
            rr = pl.ds(pl.multiple_of(r * LANES, LANES), LANES)
            x = u_ref[rr, :].astype(F32)
            n_s[rr, :] = layer_norm(x, *affine(ln_ref, layer, 2))
            acc_s[rr, :] = x + row_of(b2_ref, layer)
            return carry

        lax.fori_loop(0, tokens // LANES, body, 0)

    for m in range(tokens // chunk):
        rr = slice(m * chunk, (m + 1) * chunk)
        n = n_s[rr, :]
        p2 = dot(n, w1b_ref[0]) + row_of(b1b_ref, layer)
        p1 = dot(n, w1a_ref[0]) + row_of(b1a_ref, layer)
        half = 0.5 * p2
        gated = (p1 * (half + half * lax.erf(p2 * math.sqrt(0.5)))).astype(BF)
        acc_s[rr, :] += dot(gated, w2_ref[0])

    @pl.when(step == pl.num_programs(0) - 1)
    def _():
        out_ref[...] = acc_s[...].astype(BF)


def ffn_call(u, ln_par, w1, b1, w2, b2, layer, ft=512, chunk=512):
    tokens, chan = u.shape
    width = w2.shape[1]
    n = width // ft
    layers = w1.shape[0]
    return pl.pallas_call(
        functools.partial(ffn_kernel, layer=layer, chunk=chunk), grid=(n,),
        in_specs=[whole(u), whole(ln_par), minor((1, chan, ft), layer), pl.BlockSpec((1, chan, ft), lambda i: (layer, 0, i + n)),
                  minor((layers, ft)), pl.BlockSpec((layers, ft), lambda i: (0, i + n)),
                  pl.BlockSpec((1, ft, chan), lambda i: (layer, i, 0)), whole(b2)],
        out_specs=whole(u), out_shape=like(u.shape),
        scratch_shapes=[pltpu.VMEM(u.shape, BF), pltpu.VMEM(u.shape, F32)],
        compiler_params=params(60), cost_estimate=cost(6 * tokens * chan * width, 6 * chan * width), name="ffn")(u, ln_par, w1, w1, b1, b1, w2, b2)


def leave_kernel(core_ref, u_ref, w_ref, pb_ref, h_ref, out_ref, sum_ref, edge_ref):
    sums, squares = [], []
    core = core_ref[0]
    tok = u_ref.shape[1]
    for l in range(u_ref.shape[0]):
        y = dot(u_ref[l], w_ref[0]) + row_of(pb_ref, 1) + h_ref[l].astype(F32)
        y = y.astype(BF)
        out_ref[l] = y
        edge_ref[l] = jnp.where(core == 0, y[tok - LANES:], y[:LANES])
        y = y.astype(F32)
        sums.append(col_sum(y))
        squares.append(col_sum(y * y))
    sum_ref[...] = place_rows(sums, squares, 0)


def leave_call(core, u, proj_w, proj_b, h, nt=256):
    lat, tok, chan = u.shape
    return pl.pallas_call(
        leave_kernel,
        grid_spec=pltpu.PrefetchScalarGridSpec(
            num_scalar_prefetch=1, grid=(chan // nt,),
            in_specs=[whole(u), minor((1, chan, nt), 1), minor((2, nt)), minor((lat, tok, nt))],
            out_specs=[minor((lat, tok, nt)), minor((SUM_ROWS, nt)), minor((lat, LANES, nt))]),
        out_shape=[like(u.shape), like((SUM_ROWS, chan), F32), like((lat, LANES, chan))],
        compiler_params=params(60), cost_estimate=cost(2 * lat * tok * chan * chan, 2 * chan * chan), name="leave")(core, u, proj_w, proj_b, h)


SWAP = pairs_of('01 10 23 32')


def device_block(latents, time_emb, context, res_norm, res_conv_w, res_conv_b, res_temb_w, res_temb_b, tr_norm, proj_w, proj_b, ln_par, self_qkv, cross_q, cross_kv, attn_out, attn_b, ff_in_w, ff_in_b, ff_out_w, ff_out_b):
    index = lax.axis_index('sp')
    chip, core = index // 2, index % 2
    core_vec = jnp.reshape(core, (1,)).astype(jnp.int32)
    count, rows_n, cols, chan = latents.shape
    lat = count // 2
    tok = 2 * rows_n * cols
    ctx_len = context.shape[1]
    where = jnp.reshape(index, (1,)).astype(jnp.int32)
    flat = latents.reshape(count, rows_n * cols, chan)
    arrived = []
    for l in (2, 0, 1):
        low, high = flat[l:l + 1], flat[lat + l:lat + l + 1]
        first = lax.ppermute(jnp.where(core == 0, high, low), 'sp', pairs_of('02 10 23 31'))
        second = lax.ppermute(jnp.where(chip == 0, high, low), 'sp', pairs_of('12 21'))
        arrived.append((first, second))

    temb = lax.dynamic_slice(time_emb, (chip * lat, 0), (lat, chan))
    temb = jax.nn.silu(temb.astype(F32)).astype(BF)
    tembs = [dot(temb, res_temb_w[r]) + res_temb_b[r] for r in range(2)]
    ctx = lax.dynamic_slice(context, (chip * lat, 0, 0), (lat,) + context.shape[1:])
    ctx = jnp.pad(ctx, ((0, 0), (0, LANES - ctx_len), (0, 0)))
    ckv_t = jnp.moveaxis(cross_kv, 2, -1).reshape(cross_kv.shape[:2] + (chan, -1))
    kc, vc = context_call(ctx, ckv_t)
    qkv_t = jnp.moveaxis(self_qkv, 2, -1).reshape(self_qkv.shape[:2] + (chan, chan))
    cq_t = jnp.moveaxis(cross_q, 1, -1).reshape(-1, chan, chan)
    attn_w = attn_out.reshape(attn_b.shape[:2] + (chan, chan))
    conv_w = res_conv_w.reshape(-1, KERNEL, KERNEL * chan, chan)

    swap = lambda a: lax.ppermute(a, 'sp', SWAP)
    early, kc, vc, tembs = lax.optimization_barrier((arrived[0], kc, vc, tembs))
    v, own, edge = gather_call(where, flat, early[:1], early[1:], 2)
    into = conv_call(core_vec, v, swap(edge), own, swap(own), res_norm, res_conv_b, conv_w, 0, 0, temb=tembs[0], base=2, lat=1)
    late, v, into = lax.optimization_barrier((arrived[1:], v, into))
    v, own, edge = gather_call(where, flat, [a[0] for a in late], [a[1] for a in late], 0, into=v)
    t, sums_t, edge = conv_call(core_vec, v, swap(edge), own, swap(own), res_norm, res_conv_b, conv_w, 0, 0, temb=tembs[0], into=into, base=0, lat=2)
    h, sums_h, _ = conv_call(core_vec, t, swap(edge), sums_t, swap(sums_t), res_norm, res_conv_b, conv_w, 0, 1, res=v)
    u, n, k = enter_call(h, sums_h, swap(sums_h), tr_norm, proj_w, proj_b, ln_par, qkv_t)
    for layer in range(2):
        if layer:
            n, k = key_call(u, ln_par, qkv_t, layer)
        k_far = swap(k)
        vals = linear_call(value_kernel, n, qkv_t, layer, 2, (chan, tok), "values")
        vals_far = swap(vals)
        q = linear_call(query_kernel, n, qkv_t, layer, 0, (tok, chan), "queries")
        att = attn_call(q, k, k_far, vals, vals_far)
        u = post_call(att, u, attn_w, attn_b, ln_par, cq_t, kc, vc, layer, ctx_len)
        u = ffn_call(u.reshape(lat * tok, chan), ln_par, ff_in_w, ff_in_b, ff_out_w, ff_out_b, layer).reshape(lat, tok, chan)
    h, sums_h, edge = leave_call(core_vec, u, proj_w, proj_b, h)
    t, sums_t, edge = conv_call(core_vec, h, swap(edge), sums_h, swap(sums_h), res_norm, res_conv_b, conv_w, 1, 0, temb=tembs[1])
    edge, peer = swap(edge), swap(sums_t)
    lows, highs = [], []
    for l in range(lat):
        out = conv_call(core_vec, t, edge, sums_t, peer, res_norm, res_conv_b, conv_w, 1, 1, res=h, base=l, lat=1, want_sums=False)
        top, bottom = out[:, :tok // 2], out[:, tok // 2:]
        first = lax.ppermute(jnp.where(chip == 0, bottom, top), 'sp', pairs_of('20 01 32 13'))
        second = lax.ppermute(jnp.where(core == 0, bottom, top), 'sp', pairs_of('21 12'))
        third = jnp.where(index == 0, top, jnp.where(index == 3, bottom, second))
        lows.append(jnp.where(core == 0, third, first))
        highs.append(jnp.where(core == 0, first, third))
    return jnp.concatenate(lows + highs, axis=0).reshape(latents.shape)


def solution(mesh):
    row_spec = P('dp', 'sp')
    part_spec = P('dp')
    in_specs = (row_spec, part_spec, part_spec) + (P(),) * 18
    return jax.shard_map(device_block, mesh=mesh, in_specs=in_specs, out_specs=row_spec, check_vma=False)
```

```python
import functools
import math
import jax
import jax.numpy as jnp
from jax import lax
from jax.experimental import pallas as pl
from jax.experimental.pallas import tpu as pltpu
from jax.sharding import PartitionSpec as P

F32 = jnp.float32
BF = jnp.bfloat16
HIGHEST = lax.Precision.HIGHEST
NT = (((1,), (1,)), ((), ()))
NUM_GROUPS = 32
HEAD = 64
LANES = 128
MIB = 2 ** 20
LATENTS = 3
KERNEL = 3
WIDE = 256
CHUNKS = 2
SUM_ROWS = 8
CTX_ROWS = 80
SOFTMAX_MUL = math.log2(math.e) / math.sqrt(HEAD)

def params(mib):
    return pltpu.CompilerParams(vmem_limit_bytes=mib * MIB)


def cost(flops, nbytes):
    return pl.CostEstimate(flops=int(flops), bytes_accessed=int(nbytes), transcendentals=0)


def fixed(shape, *lead):
    index = tuple(lead) + (0,) * (len(shape) - len(lead))
    return pl.BlockSpec(tuple(shape), lambda *_: index, pipeline_mode=pl.Buffered(1))


def whole(array):
    return fixed(array.shape)


def major(shape):
    return pl.BlockSpec(tuple(shape), lambda b, *_: (b,) + (0,) * (len(shape) - 1))


def minor(shape, lead=0):
    return pl.BlockSpec(tuple(shape), lambda n, *_: (lead,) + (0,) * (len(shape) - 2) + (n,))


def any_space():
    return pl.BlockSpec(memory_space=pl.ANY)


def dot(left, right):
    return jnp.dot(left, right, preferred_element_type=F32)


def dot_nt(left, right):
    return lax.dot_general(left, right, NT, preferred_element_type=F32)


def col_sum(values):
    return jnp.sum(values, axis=0, keepdims=True)


def col_max(values):
    return jnp.max(values, axis=0, keepdims=True)


def row_of(ref, *index):
    return ref[index][None, :]


def affine(ref, *index):
    return row_of(ref, *index, 0), row_of(ref, *index, 1)


def like(array, dtype=BF):
    return jax.ShapeDtypeStruct(tuple(array), dtype)


def at_lanes(index, size=LANES):
    return slice(index * size, (index + 1) * size)


def pairs_of(text):
    return [tuple(map(int, pair)) for pair in text.split()]


def group_stats(totals, lat, count, eps):
    chan = totals.shape[1]
    per = chan // NUM_GROUPS
    fold = (lax.broadcasted_iota(jnp.int32, (chan, LANES), 0) // per == lax.broadcasted_iota(jnp.int32, (chan, LANES), 1)).astype(F32)
    spread = (lax.broadcasted_iota(jnp.int32, (LANES, chan), 1) // per == lax.broadcasted_iota(jnp.int32, (LANES, chan), 0)).astype(F32)
    grouped = jnp.dot(totals, fold, precision=HIGHEST, preferred_element_type=F32) * (1.0 / (count * per))
    means = jnp.dot(grouped, spread, precision=HIGHEST, preferred_element_type=F32)
    mean = means[0:lat]
    return mean, lax.rsqrt(means[lat:2 * lat] - mean * mean + eps)


def layer_norm(values, gain, bias):
    centered = values - jnp.mean(values, axis=-1, keepdims=True)
    variance = jnp.mean(centered * centered, axis=-1, keepdims=True)
    return (centered * lax.rsqrt(variance + 1e-5) * gain + bias).astype(BF)


def place_rows(sums, squares, base):
    zero = jnp.zeros_like(sums[0])
    rows = [zero] * SUM_ROWS
    for l, (one, two) in enumerate(zip(sums, squares)):
        rows[base + l] = one
        rows[LATENTS + base + l] = two
    return jnp.concatenate(rows, axis=0)


def conv_kernel(core_ref, v_ref, halo_ref, own_ref, peer_ref, norm_ref, bias_ref, *rest, res_i, conv_i, eps, base, has_temb, has_res, has_into, want_sums):
    rest = list(rest)
    temb_ref = rest.pop(0) if has_temb else None
    w_hbm = rest.pop(0)
    res_ref = rest.pop(0) if has_res else None
    acat, w_buf, w_sem = rest[-3:]
    rest = rest[:-3]
    before_ref = None
    if has_into:
        _, _, before_ref = rest[:3]
        rest = rest[3:]
    out_ref = rest.pop(0)
    sum_ref, edge_ref = rest if want_sums else (rest[0], None)
    lat, tok, chan = v_ref.shape
    rows = tok // LANES
    core, chip = core_ref[0] % 2, core_ref[0] // 2
    step, steps = pl.program_id(0), pl.num_programs(0)
    nt = out_ref.shape[-1]

    def fetch(n):
        lanes = pl.ds(pl.multiple_of(n * nt, LANES), nt)
        return pltpu.make_async_copy(w_hbm.at[2 * res_i + conv_i, :, :, lanes], w_buf.at[n % 2], w_sem.at[n % 2])

    @pl.when(step == 0)
    def _():
        fetch(0).start()
        fetch(1).start()
        mean, inv = group_stats(own_ref[...] + peer_ref[...], LATENTS, 2 * tok, eps)
        gain, shift = affine(norm_ref, res_i, conv_i)
        scale = inv * gain

        def emit(src, l, row, cs):
            g = base + l
            x = (src.astype(F32) - row_of(mean, g, cs)) * row_of(scale, g, cs) + shift[:, cs]
            half = 0.5 * x
            y = half * jnp.tanh(half) + half
            col = lax.broadcasted_iota(jnp.int32, y.shape, 0)
            left = jnp.where(col == 0, 0.0, pltpu.roll(y, 1, 0))
            right = jnp.where(col == LANES - 1, 0.0, pltpu.roll(y, LANES - 1, 0))
            rr = pl.ds(pl.multiple_of(row * LANES, LANES), LANES)
            for d, val in enumerate((left, y, right)):
                acat[l, rr, d * chan + cs.start:d * chan + cs.stop] = val.astype(BF)

        for l in range(lat):
            def one_row(r, carry):
                for ch in range(chan // WIDE):
                    cs = at_lanes(ch, WIDE)
                    emit(v_ref[l, pl.ds(pl.multiple_of(r * LANES, LANES), LANES), cs], l, r + 1, cs)
                return carry

            lax.fori_loop(0, rows, one_row, 0)
            for ch in range(chan // WIDE):
                cs = at_lanes(ch, WIDE)
                emit(halo_ref[l, :, cs], l, jnp.where(core == 0, rows + 1, 0), cs)
            rr = pl.ds(pl.multiple_of(jnp.where(core == 0, 0, rows + 1) * LANES, LANES), LANES)
            acat[l, rr, :] = jnp.zeros((LANES, KERNEL * chan), BF)

    slot = step % 2
    fetch(step).wait()
    sums, squares = [], []
    for l in range(lat):
        acc = row_of(bias_ref, res_i, conv_i)
        for dy in range(KERNEL):
            acc += dot(acat[l, dy * LANES:tok + dy * LANES, :], w_buf[slot, dy])
        if has_temb:
            acc += row_of(temb_ref, base + l)
        if has_res:
            acc += res_ref[l].astype(F32)
        out = acc.astype(BF)
        if want_sums:
            out_ref[l] = out
            edge_ref[l] = jnp.where(core == 0, out[tok - LANES:], out[:LANES])
            out = out.astype(F32)
            sums.append(col_sum(out))
            squares.append(col_sum(out * out))
        else:
            half = tok // 2
            out_ref[l] = jnp.where(chip == 0, out[half:], out[:half])
            sum_ref[l] = jnp.where(chip == 0, out[:half], out[half:])
    if want_sums:
        placed = place_rows(sums, squares, base)
        sum_ref[...] = placed + before_ref[...] if has_into else placed

    @pl.when(step + 2 < steps)
    def _():
        fetch(step + 2).start()


def conv_call(core, v, halo, own, peer, norm, bias, weights, res_i, conv_i, temb=None, res=None, into=None, base=0, lat=LATENTS, want_sums=True, nt=256):
    tok, chan = v.shape[1:]
    pick = lambda a: (base // lat if a.shape[0] > lat else 0)
    rows = lambda a: fixed((lat,) + a.shape[1:], pick(a))
    tile = lambda a, size: minor((lat, size, nt), pick(a))
    specs = [rows(v), rows(halo), whole(own), whole(peer), whole(norm), minor(bias.shape[:-1] + (nt,))]
    args = [v, halo, own, peer, norm, bias]
    if temb is not None:
        specs.append(minor((LATENTS, nt)))
        args.append(temb)
    specs.append(any_space())
    args.append(weights)
    if res is not None:
        specs.append(tile(res, tok))
        args.append(res)
    aliases = {}
    held = LATENTS if want_sums else lat
    out = like((held, tok if want_sums else tok // 2, chan))
    if into is not None:
        aliases = {len(args) + 1: 0, len(args) + 2: 2}
        specs += [any_space(), any_space(), minor((SUM_ROWS, nt))]
        args += [into[0], into[2], into[1]]
    out_specs, out_shape = [tile(out, out.shape[1])], [out]
    if want_sums:
        out_specs += [minor((SUM_ROWS, nt)), tile(out, LANES)]
        out_shape += [like((SUM_ROWS, chan), F32), like((held, LANES, chan))]
    else:
        out_specs, out_shape = out_specs * 2, out_shape * 2
    body = functools.partial(conv_kernel, res_i=res_i, conv_i=conv_i, eps=1e-5, base=base, has_temb=temb is not None, has_res=res is not None, has_into=into is not None, want_sums=want_sums)
    outs = pl.pallas_call(
        body,
        grid_spec=pltpu.PrefetchScalarGridSpec(
            num_scalar_prefetch=1, grid=(chan // nt,), in_specs=specs, out_specs=out_specs,
            scratch_shapes=[pltpu.VMEM((lat, tok + 2 * LANES, KERNEL * chan), BF), pltpu.VMEM((2, KERNEL, KERNEL * chan, nt), BF), pltpu.SemaphoreType.DMA((2,))]),
        out_shape=out_shape, compiler_params=params(60), input_output_aliases=aliases,
        cost_estimate=cost(18 * lat * tok * chan * chan, 18 * chan * chan), name="conv")(core, *args)
    return outs


def gather_kernel(where_ref, *rest, base, lat, has_into):
    parts = rest[:2 * lat]
    v_ref, sum_ref, edge_ref = rest[2 * lat + has_into:]
    index = where_ref[0]
    chip, core = index // 2, index % 2
    sums, squares = [], []
    for l in range(lat):
        first, second = parts[2 * l][0], parts[2 * l + 1][0]
        half = first.shape[0]
        top = jnp.where(chip == 0, second, first)
        bottom = jnp.where(chip == 0, first, second)
        v_ref[l, :half] = top
        v_ref[l, half:] = bottom
        edge_ref[l] = jnp.where(core == 0, bottom[half - LANES:], top[:LANES])
        top, bottom = top.astype(F32), bottom.astype(F32)
        sums.append(col_sum(top) + col_sum(bottom))
        squares.append(col_sum(top * top) + col_sum(bottom * bottom))
    sum_ref[...] = place_rows(sums, squares, base)


def gather_call(where, first, second, base, into=None):
    lat, half, chan = first.shape
    nt = 640
    specs, args = [], []
    for l in range(lat):
        specs += [minor((1, half, nt), l)] * 2
        args += [first, second]
    aliases = {}
    if into is not None:
        specs.append(any_space())
        args.append(into)
        aliases = {len(args): 0}
    return pl.pallas_call(
        functools.partial(gather_kernel, base=base, lat=lat, has_into=into is not None),
        grid_spec=pltpu.PrefetchScalarGridSpec(
            num_scalar_prefetch=1, grid=(chan // nt,), in_specs=specs,
            out_specs=[minor((lat, 2 * half, nt), base // lat), minor((SUM_ROWS, nt)), minor((lat, LANES, nt))]),
        out_shape=[like((LATENTS, 2 * half, chan)), like((SUM_ROWS, chan), F32), like((lat, LANES, chan))],
        input_output_aliases=aliases, compiler_params=params(60), cost_estimate=cost(MIB, 8 * lat * half * chan), name="gather")(where, *args)


def enter_kernel(h_ref, own_ref, peer_ref, norm_ref, pw_ref, pb_ref, ln_ref, wk_ref, u_ref, n_ref, k_ref, mean_s, scale_s):
    step = pl.program_id(0)
    lat = pl.num_programs(0)

    @pl.when(step == 0)
    def _():
        mean, inv = group_stats(own_ref[...] + peer_ref[...], LATENTS, 2 * h_ref.shape[1], 1e-6)
        mean_s[:LATENTS] = mean
        scale_s[:LATENTS] = inv * row_of(norm_ref, 0)

    mean, scale = mean_s[pl.ds(step, 1), :], scale_s[pl.ds(step, 1), :]
    chunks = [at_lanes(i, h_ref.shape[1] // CHUNKS) for i in range(CHUNKS)]
    tokens = []
    for rr in chunks:
        normed = ((h_ref[0, rr].astype(F32) - mean) * scale + row_of(norm_ref, 1)).astype(BF)
        tokens.append((dot(normed, pw_ref[0]) + row_of(pb_ref, 0)).astype(BF))
    for rr, u in zip(chunks, tokens):
        u_ref[0, rr] = u
        n = layer_norm(u.astype(F32), *affine(ln_ref, 0, 0))
        n_ref[0, rr] = n
        k_ref[0, rr] = dot_nt(n, wk_ref[0, 0]).astype(BF)


def enter_call(h, own, peer, tr_norm, proj_w, proj_b, ln_par, qkv_t):
    lat, tok, chan = h.shape
    row = major((1, tok, chan))
    return pl.pallas_call(
        enter_kernel, grid=(lat,),
        in_specs=[row, whole(own), whole(peer), whole(tr_norm), fixed((1, chan, chan)), whole(proj_b), whole(ln_par), fixed((1, 1, chan, chan), 0, 1)],
        out_specs=[row] * 3, out_shape=[like(h.shape)] * 3,
        scratch_shapes=[pltpu.VMEM((SUM_ROWS, chan), F32)] * 2,
        compiler_params=params(60), cost_estimate=cost(4 * lat * tok * chan * chan, 4 * chan * chan), name="enter")(
            h, own, peer, tr_norm, proj_w, proj_b, ln_par, qkv_t)


def key_kernel(u_ref, ln_ref, wk_ref, n_ref, k_ref, *, layer):
    for i in range(CHUNKS):
        rr = at_lanes(i, u_ref.shape[1] // CHUNKS)
        n = layer_norm(u_ref[0, rr].astype(F32), *affine(ln_ref, layer, 0))
        n_ref[0, rr] = n
        k_ref[0, rr] = dot_nt(n, wk_ref[0, 0]).astype(BF)


def key_call(u, ln_par, qkv_t, layer):
    lat, tok, chan = u.shape
    row = major((1, tok, chan))
    return pl.pallas_call(
        functools.partial(key_kernel, layer=layer), grid=(lat,),
        in_specs=[row, whole(ln_par), fixed((1, 1, chan, chan), layer, 1)],
        out_specs=[row] * 2, out_shape=[like(u.shape)] * 2,
        compiler_params=params(60), cost_estimate=cost(2 * lat * tok * chan * chan, 2 * chan * chan), name="keys")(u, ln_par, qkv_t)


def query_kernel(n_ref, w_ref, q_ref):
    q_ref[0] = dot_nt(n_ref[0], w_ref[0, 0]).astype(BF)


def value_kernel(n_ref, w_ref, v_ref):
    v_ref[0] = dot_nt(w_ref[0, 0], n_ref[0]).astype(BF)


def linear_call(kernel, n, qkv_t, layer, part, out_block, name):
    lat, tok, chan = n.shape
    return pl.pallas_call(
        kernel, grid=(lat,),
        in_specs=[major((1, tok, chan)), fixed((1, 1, chan, chan), layer, part)],
        out_specs=major((1,) + out_block), out_shape=like((lat,) + out_block),
        compiler_params=params(60), cost_estimate=cost(tok * chan * chan // 4, 2 * chan * chan), name=name)(n, qkv_t)


def attn_kernel(q_ref, k0_ref, k1_ref, v0_ref, v1_ref, o_ref, *, pairs):
    def scores(i):
        p, h = divmod(i, 2)
        ls = slice(p * LANES, (p + 1) * LANES)
        q = q_ref[0, :, ls]
        lane = lax.broadcasted_iota(jnp.int32, q.shape, 1)
        qh = jnp.where((lane >= HEAD) == (h == 1), q, jnp.zeros_like(q))
        return [dot_nt(k_ref[0, :, ls], qh) for k_ref in (k0_ref, k1_ref)]

    coming = scores(0)
    halves = []
    for i in range(2 * pairs):
        s0, s1 = coming
        if i + 1 < 2 * pairs:
            coming = scores(i + 1)
        top = jnp.maximum(col_max(s0), col_max(s1))
        vs = slice(i * HEAD, (i + 1) * HEAD)
        e0 = jnp.exp2((s0 - top) * SOFTMAX_MUL)
        o = jnp.dot(v0_ref[0, vs, :], e0.astype(BF), preferred_element_type=F32)
        total = col_sum(e0)
        e1 = jnp.exp2((s1 - top) * SOFTMAX_MUL)
        o += jnp.dot(v1_ref[0, vs, :], e1.astype(BF), preferred_element_type=F32)
        total += col_sum(e1)
        halves.append(o / total)
        if i % 2:
            p = i // 2
            o_ref[0, :, p * LANES:(p + 1) * LANES] = jnp.transpose(jnp.concatenate(halves, axis=0)).astype(BF)
            halves = []


def attn_call(q, k0, k1, v0, v1, pairs=5):
    lat, tok, chan = q.shape
    width = LANES * pairs
    qs = pl.BlockSpec((1, tok, width), lambda b, h: (b, 0, h))
    vs = pl.BlockSpec((1, width, tok), lambda b, h: (b, h, 0))
    return pl.pallas_call(
        functools.partial(attn_kernel, pairs=pairs), grid=(lat, chan // width), in_specs=[qs, qs, qs, vs, vs], out_specs=qs,
        out_shape=like(q.shape), compiler_params=params(60),
        cost_estimate=cost(8 * lat * tok * tok * chan, 12 * lat * tok * chan), name="attn")(q, k0, k1, v0, v1)


def context_kernel(ctx_ref, w_ref, k_ref, v_ref):
    lat, padded, depth = ctx_ref.shape
    tokens = ctx_ref[...].reshape(lat * padded, depth)
    keys = dot_nt(tokens, w_ref[0, 0]).astype(BF)
    values = dot_nt(w_ref[0, 1], tokens).astype(BF)
    for l in range(lat):
        k_ref[0, l] = keys[l * padded:l * padded + CTX_ROWS]
        v_ref[0, l] = values[:, at_lanes(l, padded)]


def context_call(ctx, ckv_t):
    lat, padded, depth = ctx.shape
    layers, _, chan, _ = ckv_t.shape
    return pl.pallas_call(
        context_kernel, grid=(layers,),
        in_specs=[whole(ctx), major((1, 2, chan, depth))],
        out_specs=[major((1, lat, CTX_ROWS, chan)), major((1, lat, chan, padded))],
        out_shape=[like((layers, lat, CTX_ROWS, chan)), like((layers, lat, chan, padded))],
        compiler_params=params(60), cost_estimate=cost(4 * layers * lat * padded * depth * chan, 4 * layers * depth * chan), name="context")(ctx, ckv_t)


def cross_attend(q_s, kc_ref, vc_ref, o_s, ctx_len):
    tok, chan = q_s.shape

    def scores(p):
        kc = kc_ref[0, 0, :, at_lanes(p)]
        lane = lax.broadcasted_iota(jnp.int32, kc.shape, 1)
        zero = jnp.zeros_like(kc)
        both = jnp.concatenate([jnp.where(lane < HEAD, kc, zero), jnp.where(lane >= HEAD, kc, zero)], axis=0)
        return dot_nt(both, q_s[:, at_lanes(p)])

    pairs = chan // LANES
    coming = scores(0)
    for p in range(pairs):
        s = coming
        if p + 1 < pairs:
            coming = scores(p + 1)
        exps, sums = [], []
        for h in range(2):
            sh = s[at_lanes(h, CTX_ROWS)]
            valid = lax.broadcasted_iota(jnp.int32, sh.shape, 0) < ctx_len
            sh = jnp.where(valid, sh, -jnp.inf)
            e = jnp.exp2((sh - col_max(sh)) * SOFTMAX_MUL)
            sums.append(col_sum(e))
            exps += [e.astype(BF), jnp.zeros((LANES - CTX_ROWS, tok), BF)]
        vc = vc_ref[0, 0, at_lanes(p), :]
        row = lax.broadcasted_iota(jnp.int32, vc.shape, 0)
        zero = jnp.zeros_like(vc)
        vb = jnp.concatenate([jnp.where(row < HEAD, vc, zero), jnp.where(row >= HEAD, vc, zero)], axis=1)
        o = dot(vb, jnp.concatenate(exps, axis=0))
        o = jnp.concatenate([o[:HEAD] / sums[0], o[HEAD:] / sums[1]], axis=0)
        o_s[:, at_lanes(p)] = jnp.transpose(o).astype(BF)


def rest_kernel(att_ref, u_ref, wo_ref, ab_ref, ln_ref, wq_ref, kc_ref, vc_ref, wc_ref, w1a_ref, w1b_ref, b1a_ref, b1b_ref, w2_ref, b2_ref, out_ref, q_s, o_s, u_s, n_s, acc_s, *, layer, ctx_len, lat, chunk):
    step = pl.program_id(0)
    tok = u_ref.shape[1]
    chunks = [at_lanes(i, tok // CHUNKS) for i in range(CHUNKS)]

    @pl.when(step < lat)
    def _():
        for rr in chunks:
            u_s[rr] = (dot(att_ref[0, rr], wo_ref[0, 0]) + u_ref[0, rr].astype(F32) + row_of(ab_ref, layer, 0)).astype(BF)
        for rr in chunks:
            q_s[rr] = dot_nt(layer_norm(u_s[rr].astype(F32), *affine(ln_ref, layer, 1)), wq_ref[0]).astype(BF)
        cross_attend(q_s, kc_ref, vc_ref, o_s, ctx_len)
        for rr in chunks:
            y = (dot(o_s[rr], wc_ref[0, 0]) + u_s[rr].astype(F32) + row_of(ab_ref, layer, 1)).astype(BF).astype(F32)
            rows = pl.ds(pl.multiple_of(step * tok + rr.start, LANES), rr.stop - rr.start)
            n_s[rows] = layer_norm(y, *affine(ln_ref, layer, 2))
            acc_s[rows] = y + row_of(b2_ref, layer)

    @pl.when(step >= lat)
    def _():
        for m in range(n_s.shape[0] // chunk):
            rr = at_lanes(m, chunk)
            n = n_s[rr]
            p2 = dot(n, w1b_ref[0]) + row_of(b1b_ref, layer)
            p1 = dot(n, w1a_ref[0]) + row_of(b1a_ref, layer)
            half = 0.5 * p2
            gated = (p1 * (half + half * lax.erf(p2 * math.sqrt(0.5)))).astype(BF)
            acc_s[rr] += dot(gated, w2_ref[0])

    @pl.when(step == pl.num_programs(0) - 1)
    def _():
        out_ref[...] = acc_s[...].astype(BF)


def rest_call(att, u, attn_out, attn_b, ln_par, cq_t, kc, vc, w1, b1, w2, b2, layer, ctx_len, ft=512, chunk=512):
    lat, tok, chan = u.shape
    width = w2.shape[1]
    n = width // ft
    row = pl.BlockSpec((1, tok, chan), lambda i: (jnp.minimum(i, lat - 1), 0, 0))
    ctx_spec = lambda a: pl.BlockSpec((1, 1) + a.shape[2:], lambda i: (layer, jnp.minimum(i, lat - 1), 0, 0))
    mat = lambda i: fixed((1, 1, chan, chan), layer, i)
    part = lambda i: jnp.maximum(i - lat, 0)
    flat = (lat * tok, chan)
    return pl.pallas_call(
        functools.partial(rest_kernel, layer=layer, ctx_len=ctx_len, lat=lat, chunk=chunk), grid=(lat + n,),
        in_specs=[row, row, mat(0), whole(attn_b), whole(ln_par), fixed((1, chan, chan), layer), ctx_spec(kc), ctx_spec(vc), mat(1),
                  pl.BlockSpec((1, chan, ft), lambda i: (layer, 0, part(i))), pl.BlockSpec((1, chan, ft), lambda i: (layer, 0, part(i) + n)),
                  pl.BlockSpec((w1.shape[0], ft), lambda i: (0, part(i))), pl.BlockSpec((w1.shape[0], ft), lambda i: (0, part(i) + n)),
                  pl.BlockSpec((1, ft, chan), lambda i: (layer, part(i), 0)), whole(b2)],
        out_specs=fixed(flat), out_shape=like(flat),
        scratch_shapes=[pltpu.VMEM((tok, chan), BF)] * 3 + [pltpu.VMEM(flat, BF), pltpu.VMEM(flat, F32)],
        compiler_params=params(62), cost_estimate=cost(6 * lat * tok * chan * (chan + width), 6 * chan * (chan + width)), name="rest")(
            att, u, attn_out, attn_b, ln_par, cq_t, kc, vc, attn_out, w1, w1, b1, b1, w2, b2)


def leave_kernel(core_ref, u_ref, w_ref, pb_ref, h_ref, out_ref, sum_ref, edge_ref):
    sums, squares = [], []
    core = core_ref[0]
    tok = u_ref.shape[1]
    for l in range(u_ref.shape[0]):
        y = dot(u_ref[l], w_ref[0]) + row_of(pb_ref, 1) + h_ref[l].astype(F32)
        y = y.astype(BF)
        out_ref[l] = y
        edge_ref[l] = jnp.where(core == 0, y[tok - LANES:], y[:LANES])
        y = y.astype(F32)
        sums.append(col_sum(y))
        squares.append(col_sum(y * y))
    sum_ref[...] = place_rows(sums, squares, 0)


def leave_call(core, u, proj_w, proj_b, h, nt=256):
    lat, tok, chan = u.shape
    return pl.pallas_call(
        leave_kernel,
        grid_spec=pltpu.PrefetchScalarGridSpec(
            num_scalar_prefetch=1, grid=(chan // nt,),
            in_specs=[whole(u), minor((1, chan, nt), 1), minor((2, nt)), minor((lat, tok, nt))],
            out_specs=[minor((lat, tok, nt)), minor((SUM_ROWS, nt)), minor((lat, LANES, nt))]),
        out_shape=[like(u.shape), like((SUM_ROWS, chan), F32), like((lat, LANES, chan))],
        compiler_params=params(60), cost_estimate=cost(2 * lat * tok * chan * chan, 2 * chan * chan), name="leave")(core, u, proj_w, proj_b, h)


SWAP = pairs_of('01 10 23 32')


def device_block(latents, time_emb, context, res_norm, res_conv_w, res_conv_b, res_temb_w, res_temb_b, tr_norm, proj_w, proj_b, ln_par, self_qkv, cross_q, cross_kv, attn_out, attn_b, ff_in_w, ff_in_b, ff_out_w, ff_out_b):
    index = lax.axis_index('sp')
    chip, core = index // 2, index % 2
    core_vec = jnp.reshape(core, (1,)).astype(jnp.int32)
    count, rows_n, cols, chan = latents.shape
    lat = count // 2
    tok = 2 * rows_n * cols
    ctx_len = context.shape[1]
    where = jnp.reshape(index, (1,)).astype(jnp.int32)
    flat = latents.reshape(count, rows_n * cols, chan)
    halves = flat.reshape(2, lat, rows_n * cols, chan)
    going, staying = lax.dynamic_index_in_dim(halves, 1 - core, keepdims=False), lax.dynamic_index_in_dim(halves, core, keepdims=False)

    def spread(part):
        return lax.ppermute(going[part], 'sp', pairs_of('02 10 23 31')), lax.ppermute(staying[part], 'sp', pairs_of('12 21 00 33'))

    early, late = spread(slice(lat - 1, lat)), spread(slice(0, lat - 1))

    temb = lax.dynamic_slice(time_emb, (chip * lat, 0), (lat, chan))
    temb = jax.nn.silu(temb.astype(F32)).astype(BF)
    tembs = [dot(temb, res_temb_w[r]) + res_temb_b[r] for r in range(2)]
    ctx = lax.dynamic_slice(context, (chip * lat, 0, 0), (lat,) + context.shape[1:])
    ctx = jnp.pad(ctx, ((0, 0), (0, LANES - ctx_len), (0, 0)))
    ckv_t = jnp.moveaxis(cross_kv, 2, -1).reshape(cross_kv.shape[:2] + (chan, -1))
    kc, vc = context_call(ctx, ckv_t)
    qkv_t = jnp.moveaxis(self_qkv, 2, -1).reshape(self_qkv.shape[:2] + (chan, chan))
    cq_t = jnp.moveaxis(cross_q, 1, -1).reshape(-1, chan, chan)
    attn_w = attn_out.reshape(attn_b.shape[:2] + (chan, chan))
    conv_w = res_conv_w.reshape(-1, KERNEL, KERNEL * chan, chan)

    swap = lambda a: lax.ppermute(a, 'sp', SWAP)
    early, kc, vc, tembs = lax.optimization_barrier((early, kc, vc, tembs))
    v, own, edge = gather_call(where, *early, 2)
    into = conv_call(where, v, swap(edge), own, swap(own), res_norm, res_conv_b, conv_w, 0, 0, temb=tembs[0], base=2, lat=1)
    late, v, into = lax.optimization_barrier((late, v, into))
    v, own, edge = gather_call(where, *late, 0, into=v)
    t, sums_t, edge = conv_call(where, v, swap(edge), own, swap(own), res_norm, res_conv_b, conv_w, 0, 0, temb=tembs[0], into=into, base=0, lat=2)
    h, sums_h, _ = conv_call(where, t, swap(edge), sums_t, swap(sums_t), res_norm, res_conv_b, conv_w, 0, 1, res=v)
    u, n, k = enter_call(h, sums_h, swap(sums_h), tr_norm, proj_w, proj_b, ln_par, qkv_t)
    for layer in range(2):
        if layer:
            n, k = key_call(u, ln_par, qkv_t, layer)
        k_far = swap(k)
        vals = linear_call(value_kernel, n, qkv_t, layer, 2, (chan, tok), "values")
        vals_far = swap(vals)
        q = linear_call(query_kernel, n, qkv_t, layer, 0, (tok, chan), "queries")
        att = attn_call(q, k, k_far, vals, vals_far)
        u = rest_call(att, u, attn_w, attn_b, ln_par, cq_t, kc, vc, ff_in_w, ff_in_b, ff_out_w, ff_out_b, layer, ctx_len).reshape(lat, tok, chan)
    h, sums_h, edge = leave_call(core_vec, u, proj_w, proj_b, h)
    t, sums_t, edge = conv_call(where, h, swap(edge), sums_h, swap(sums_h), res_norm, res_conv_b, conv_w, 1, 0, temb=tembs[1])
    edge, peer = swap(edge), swap(sums_t)
    lows, highs = [], []
    for l in range(lat):
        going, staying = conv_call(where, t, edge, sums_t, peer, res_norm, res_conv_b, conv_w, 1, 1, res=h, base=l, lat=1, want_sums=False)
        first = lax.ppermute(going, 'sp', pairs_of('20 01 32 13'))
        third = lax.ppermute(staying, 'sp', pairs_of('21 12 00 33'))
        lows.append(jnp.where(core == 0, third, first))
        highs.append(jnp.where(core == 0, first, third))
    return jnp.concatenate(lows + highs, axis=0).reshape(latents.shape)


def solution(mesh):
    row_spec = P('dp', 'sp')
    part_spec = P('dp')
    in_specs = (row_spec, part_spec, part_spec) + (P(),) * 18
    return jax.shard_map(device_block, mesh=mesh, in_specs=in_specs, out_specs=row_spec, check_vma=False)
```

```python
import functools
import math
import jax
import jax.numpy as jnp
from jax import lax
from jax.experimental import pallas as pl
from jax.experimental.pallas import tpu as pltpu
from jax.sharding import PartitionSpec as P

F32 = jnp.float32
BF = jnp.bfloat16
HIGHEST = lax.Precision.HIGHEST
NT = (((1,), (1,)), ((), ()))
NUM_GROUPS = 32
HEAD = 64
LANES = 128
MIB = 2 ** 20
LATENTS = 3
KERNEL = 3
WIDE = 256
CHUNKS = 2
SUM_ROWS = 8
CTX_ROWS = 80
SOFTMAX_MUL = math.log2(math.e) / math.sqrt(HEAD)

def params(mib):
    return pltpu.CompilerParams(vmem_limit_bytes=mib * MIB)


def cost(flops, nbytes):
    return pl.CostEstimate(flops=int(flops), bytes_accessed=int(nbytes), transcendentals=0)


def fixed(shape, *lead):
    index = tuple(lead) + (0,) * (len(shape) - len(lead))
    return pl.BlockSpec(tuple(shape), lambda *_: index, pipeline_mode=pl.Buffered(1))


def whole(array):
    return fixed(array.shape)


def major(shape):
    return pl.BlockSpec(tuple(shape), lambda b, *_: (b,) + (0,) * (len(shape) - 1))


def minor(shape, lead=0):
    return pl.BlockSpec(tuple(shape), lambda n, *_: (lead,) + (0,) * (len(shape) - 2) + (n,))


def any_space():
    return pl.BlockSpec(memory_space=pl.ANY)


def dot(left, right):
    return jnp.dot(left, right, preferred_element_type=F32)


def dot_nt(left, right):
    return lax.dot_general(left, right, NT, preferred_element_type=F32)


def col_sum(values):
    return jnp.sum(values, axis=0, keepdims=True)


def col_max(values):
    return jnp.max(values, axis=0, keepdims=True)


def row_of(ref, *index):
    return ref[index][None, :]


def affine(ref, *index):
    return row_of(ref, *index, 0), row_of(ref, *index, 1)


def like(array, dtype=BF):
    return jax.ShapeDtypeStruct(tuple(array), dtype)


def at_lanes(index, size=LANES):
    return slice(index * size, (index + 1) * size)


def pairs_of(text):
    return [tuple(map(int, pair)) for pair in text.split()]


def group_stats(totals, lat, count, eps):
    chan = totals.shape[1]
    per = chan // NUM_GROUPS
    fold = (lax.broadcasted_iota(jnp.int32, (chan, LANES), 0) // per == lax.broadcasted_iota(jnp.int32, (chan, LANES), 1)).astype(F32)
    spread = (lax.broadcasted_iota(jnp.int32, (LANES, chan), 1) // per == lax.broadcasted_iota(jnp.int32, (LANES, chan), 0)).astype(F32)
    grouped = jnp.dot(totals, fold, precision=HIGHEST, preferred_element_type=F32) * (1.0 / (count * per))
    means = jnp.dot(grouped, spread, precision=HIGHEST, preferred_element_type=F32)
    mean = means[0:lat]
    return mean, lax.rsqrt(means[lat:2 * lat] - mean * mean + eps)


def layer_norm(values, gain, bias):
    centered = values - jnp.mean(values, axis=-1, keepdims=True)
    variance = jnp.mean(centered * centered, axis=-1, keepdims=True)
    return (centered * lax.rsqrt(variance + 1e-5) * gain + bias).astype(BF)


def place_rows(sums, squares, base):
    zero = jnp.zeros_like(sums[0])
    rows = [zero] * SUM_ROWS
    for l, (one, two) in enumerate(zip(sums, squares)):
        rows[base + l] = one
        rows[LATENTS + base + l] = two
    return jnp.concatenate(rows, axis=0)


def conv_kernel(core_ref, v_ref, halo_ref, own_ref, peer_ref, norm_ref, bias_ref, *rest, res_i, conv_i, eps, base, has_temb, has_res, has_into, want_sums):
    rest = list(rest)
    temb_ref = rest.pop(0) if has_temb else None
    w_hbm = rest.pop(0)
    res_ref = rest.pop(0) if has_res else None
    acat, w_buf, w_sem = rest[-3:]
    rest = rest[:-3]
    before_ref = None
    if has_into:
        _, _, before_ref = rest[:3]
        rest = rest[3:]
    out_ref = rest.pop(0)
    sum_ref, edge_ref = rest if want_sums else (rest[0], None)
    lat, tok, chan = v_ref.shape
    rows = tok // LANES
    core, chip = core_ref[0] % 2, core_ref[0] // 2
    step, steps = pl.program_id(0), pl.num_programs(0)
    nt = out_ref.shape[-1]

    def fetch(n):
        lanes = pl.ds(pl.multiple_of(n * nt, LANES), nt)
        return pltpu.make_async_copy(w_hbm.at[2 * res_i + conv_i, :, :, lanes], w_buf.at[n % 2], w_sem.at[n % 2])

    @pl.when(step == 0)
    def _():
        fetch(0).start()
        fetch(1).start()
        mean, inv = group_stats(own_ref[...] + peer_ref[...], LATENTS, 2 * tok, eps)
        gain, shift = affine(norm_ref, res_i, conv_i)
        scale = inv * gain

        def emit(src, l, row, cs):
            g = base + l
            x = (src.astype(F32) - row_of(mean, g, cs)) * row_of(scale, g, cs) + shift[:, cs]
            half = 0.5 * x
            y = half * jnp.tanh(half) + half
            col = lax.broadcasted_iota(jnp.int32, y.shape, 0)
            left = jnp.where(col == 0, 0.0, pltpu.roll(y, 1, 0))
            right = jnp.where(col == LANES - 1, 0.0, pltpu.roll(y, LANES - 1, 0))
            rr = pl.ds(pl.multiple_of(row * LANES, LANES), LANES)
            for d, val in enumerate((left, y, right)):
                acat[l, rr, d * chan + cs.start:d * chan + cs.stop] = val.astype(BF)

        for l in range(lat):
            def one_row(r, carry):
                for ch in range(chan // WIDE):
                    cs = at_lanes(ch, WIDE)
                    emit(v_ref[l, pl.ds(pl.multiple_of(r * LANES, LANES), LANES), cs], l, r + 1, cs)
                return carry

            lax.fori_loop(0, rows, one_row, 0)
            for ch in range(chan // WIDE):
                cs = at_lanes(ch, WIDE)
                emit(halo_ref[l, :, cs], l, jnp.where(core == 0, rows + 1, 0), cs)
            rr = pl.ds(pl.multiple_of(jnp.where(core == 0, 0, rows + 1) * LANES, LANES), LANES)
            acat[l, rr, :] = jnp.zeros((LANES, KERNEL * chan), BF)

    slot = step % 2
    fetch(step).wait()
    sums, squares = [], []
    for l in range(lat):
        acc = row_of(bias_ref, res_i, conv_i)
        for dy in range(KERNEL):
            acc += dot(acat[l, dy * LANES:tok + dy * LANES, :], w_buf[slot, dy])
        if has_temb:
            acc += row_of(temb_ref, base + l)
        if has_res:
            acc += res_ref[l].astype(F32)
        out = acc.astype(BF)
        if want_sums:
            out_ref[l] = out
            edge_ref[l] = jnp.where(core == 0, out[tok - LANES:], out[:LANES])
            out = out.astype(F32)
            sums.append(col_sum(out))
            squares.append(col_sum(out * out))
        else:
            half = tok // 2
            out_ref[l] = jnp.where(chip == 0, out[half:], out[:half])
            sum_ref[l] = jnp.where(chip == 0, out[:half], out[half:])
    if want_sums:
        placed = place_rows(sums, squares, base)
        sum_ref[...] = placed + before_ref[...] if has_into else placed

    @pl.when(step + 2 < steps)
    def _():
        fetch(step + 2).start()


def conv_call(core, v, halo, own, peer, norm, bias, weights, res_i, conv_i, temb=None, res=None, into=None, base=0, lat=LATENTS, want_sums=True, nt=256):
    tok, chan = v.shape[1:]
    pick = lambda a: (base // lat if a.shape[0] > lat else 0)
    rows = lambda a: fixed((lat,) + a.shape[1:], pick(a))
    tile = lambda a, size: minor((lat, size, nt), pick(a))
    specs = [rows(v), rows(halo), whole(own), whole(peer), whole(norm), minor(bias.shape[:-1] + (nt,))]
    args = [v, halo, own, peer, norm, bias]
    if temb is not None:
        specs.append(minor((LATENTS, nt)))
        args.append(temb)
    specs.append(any_space())
    args.append(weights)
    if res is not None:
        specs.append(tile(res, tok))
        args.append(res)
    aliases = {}
    held = LATENTS if want_sums else lat
    out = like((held, tok if want_sums else tok // 2, chan))
    if into is not None:
        aliases = {len(args) + 1: 0, len(args) + 2: 2}
        specs += [any_space(), any_space(), minor((SUM_ROWS, nt))]
        args += [into[0], into[2], into[1]]
    out_specs, out_shape = [tile(out, out.shape[1])], [out]
    if want_sums:
        out_specs += [minor((SUM_ROWS, nt)), tile(out, LANES)]
        out_shape += [like((SUM_ROWS, chan), F32), like((held, LANES, chan))]
    else:
        out_specs, out_shape = out_specs * 2, out_shape * 2
    body = functools.partial(conv_kernel, res_i=res_i, conv_i=conv_i, eps=1e-5, base=base, has_temb=temb is not None, has_res=res is not None, has_into=into is not None, want_sums=want_sums)
    outs = pl.pallas_call(
        body,
        grid_spec=pltpu.PrefetchScalarGridSpec(
            num_scalar_prefetch=1, grid=(chan // nt,), in_specs=specs, out_specs=out_specs,
            scratch_shapes=[pltpu.VMEM((lat, tok + 2 * LANES, KERNEL * chan), BF), pltpu.VMEM((2, KERNEL, KERNEL * chan, nt), BF), pltpu.SemaphoreType.DMA((2,))]),
        out_shape=out_shape, compiler_params=params(60), input_output_aliases=aliases,
        cost_estimate=cost(18 * lat * tok * chan * chan, 18 * chan * chan), name="conv")(core, *args)
    return outs


def gather_kernel(where_ref, *rest, base, lat, has_into):
    parts = rest[:2 * lat]
    v_ref, sum_ref, edge_ref = rest[2 * lat + has_into:]
    index = where_ref[0]
    chip, core = index // 2, index % 2
    sums, squares = [], []
    for l in range(lat):
        first, second = parts[2 * l][0], parts[2 * l + 1][0]
        half = first.shape[0]
        top = jnp.where(chip == 0, second, first)
        bottom = jnp.where(chip == 0, first, second)
        v_ref[l, :half] = top
        v_ref[l, half:] = bottom
        edge_ref[l] = jnp.where(core == 0, bottom[half - LANES:], top[:LANES])
        top, bottom = top.astype(F32), bottom.astype(F32)
        sums.append(col_sum(top) + col_sum(bottom))
        squares.append(col_sum(top * top) + col_sum(bottom * bottom))
    sum_ref[...] = place_rows(sums, squares, base)


def gather_call(where, first, second, base, into=None):
    lat, half, chan = first.shape
    nt = 640
    specs, args = [], []
    for l in range(lat):
        specs += [minor((1, half, nt), l)] * 2
        args += [first, second]
    aliases = {}
    if into is not None:
        specs.append(any_space())
        args.append(into)
        aliases = {len(args): 0}
    return pl.pallas_call(
        functools.partial(gather_kernel, base=base, lat=lat, has_into=into is not None),
        grid_spec=pltpu.PrefetchScalarGridSpec(
            num_scalar_prefetch=1, grid=(chan // nt,), in_specs=specs,
            out_specs=[minor((lat, 2 * half, nt), base // lat), minor((SUM_ROWS, nt)), minor((lat, LANES, nt))]),
        out_shape=[like((LATENTS, 2 * half, chan)), like((SUM_ROWS, chan), F32), like((lat, LANES, chan))],
        input_output_aliases=aliases, compiler_params=params(60), cost_estimate=cost(MIB, 8 * lat * half * chan), name="gather")(where, *args)


def enter_kernel(h_ref, own_ref, peer_ref, norm_ref, pw_ref, pb_ref, ln_ref, wk_ref, u_ref, n_ref, k_ref, mean_s, scale_s):
    step = pl.program_id(0)
    lat = pl.num_programs(0)

    @pl.when(step == 0)
    def _():
        mean, inv = group_stats(own_ref[...] + peer_ref[...], LATENTS, 2 * h_ref.shape[1], 1e-6)
        mean_s[:LATENTS] = mean
        scale_s[:LATENTS] = inv * row_of(norm_ref, 0)

    mean, scale = mean_s[pl.ds(step, 1), :], scale_s[pl.ds(step, 1), :]
    chunks = [at_lanes(i, h_ref.shape[1] // CHUNKS) for i in range(CHUNKS)]
    tokens = []
    for rr in chunks:
        normed = ((h_ref[0, rr].astype(F32) - mean) * scale + row_of(norm_ref, 1)).astype(BF)
        tokens.append((dot(normed, pw_ref[0]) + row_of(pb_ref, 0)).astype(BF))
    for rr, u in zip(chunks, tokens):
        u_ref[0, rr] = u
        n = layer_norm(u.astype(F32), *affine(ln_ref, 0, 0))
        n_ref[0, rr] = n
        k_ref[0, rr] = dot_nt(n, wk_ref[0, 0]).astype(BF)


def enter_call(h, own, peer, tr_norm, proj_w, proj_b, ln_par, qkv_t):
    lat, tok, chan = h.shape
    row = major((1, tok, chan))
    return pl.pallas_call(
        enter_kernel, grid=(lat,),
        in_specs=[row, whole(own), whole(peer), whole(tr_norm), fixed((1, chan, chan)), whole(proj_b), whole(ln_par), fixed((1, 1, chan, chan), 0, 1)],
        out_specs=[row] * 3, out_shape=[like(h.shape)] * 3,
        scratch_shapes=[pltpu.VMEM((SUM_ROWS, chan), F32)] * 2,
        compiler_params=params(60), cost_estimate=cost(4 * lat * tok * chan * chan, 4 * chan * chan), name="enter")(
            h, own, peer, tr_norm, proj_w, proj_b, ln_par, qkv_t)


def key_kernel(u_ref, ln_ref, wk_ref, n_ref, k_ref, *, layer):
    for i in range(CHUNKS):
        rr = at_lanes(i, u_ref.shape[1] // CHUNKS)
        n = layer_norm(u_ref[0, rr].astype(F32), *affine(ln_ref, layer, 0))
        n_ref[0, rr] = n
        k_ref[0, rr] = dot_nt(n, wk_ref[0, 0]).astype(BF)


def key_call(u, ln_par, qkv_t, layer):
    lat, tok, chan = u.shape
    row = major((1, tok, chan))
    return pl.pallas_call(
        functools.partial(key_kernel, layer=layer), grid=(lat,),
        in_specs=[row, whole(ln_par), fixed((1, 1, chan, chan), layer, 1)],
        out_specs=[row] * 2, out_shape=[like(u.shape)] * 2,
        compiler_params=params(60), cost_estimate=cost(2 * lat * tok * chan * chan, 2 * chan * chan), name="keys")(u, ln_par, qkv_t)


def query_kernel(n_ref, w_ref, q_ref):
    q_ref[0] = dot_nt(n_ref[0], w_ref[0, 0]).astype(BF)


def value_kernel(n_ref, w_ref, v_ref):
    v_ref[0] = dot_nt(w_ref[0, 0], n_ref[0]).astype(BF)


def linear_call(kernel, n, qkv_t, layer, part, out_block, name):
    lat, tok, chan = n.shape
    return pl.pallas_call(
        kernel, grid=(lat,),
        in_specs=[major((1, tok, chan)), fixed((1, 1, chan, chan), layer, part)],
        out_specs=major((1,) + out_block), out_shape=like((lat,) + out_block),
        compiler_params=params(60), cost_estimate=cost(tok * chan * chan // 4, 2 * chan * chan), name=name)(n, qkv_t)


def attn_kernel(q_ref, k0_ref, k1_ref, v0_ref, v1_ref, o_ref, *, pairs):
    def scores(i):
        p, h = divmod(i, 2)
        ls = slice(p * LANES, (p + 1) * LANES)
        q = q_ref[0, :, ls]
        lane = lax.broadcasted_iota(jnp.int32, q.shape, 1)
        qh = jnp.where((lane >= HEAD) == (h == 1), q, jnp.zeros_like(q))
        return [dot_nt(k_ref[0, :, ls], qh) for k_ref in (k0_ref, k1_ref)]

    coming = scores(0)
    halves = []
    for i in range(2 * pairs):
        s0, s1 = coming
        if i + 1 < 2 * pairs:
            coming = scores(i + 1)
        top = jnp.maximum(col_max(s0), col_max(s1))
        vs = slice(i * HEAD, (i + 1) * HEAD)
        e0 = jnp.exp2((s0 - top) * SOFTMAX_MUL)
        o = jnp.dot(v0_ref[0, vs, :], e0.astype(BF), preferred_element_type=F32)
        total = col_sum(e0)
        e1 = jnp.exp2((s1 - top) * SOFTMAX_MUL)
        o += jnp.dot(v1_ref[0, vs, :], e1.astype(BF), preferred_element_type=F32)
        total += col_sum(e1)
        halves.append(o / total)
        if i % 2:
            p = i // 2
            o_ref[0, :, p * LANES:(p + 1) * LANES] = jnp.transpose(jnp.concatenate(halves, axis=0)).astype(BF)
            halves = []


def attn_call(q, k0, k1, v0, v1, pairs=5):
    lat, tok, chan = q.shape
    width = LANES * pairs
    qs = pl.BlockSpec((1, tok, width), lambda b, h: (b, 0, h))
    vs = pl.BlockSpec((1, width, tok), lambda b, h: (b, h, 0))
    return pl.pallas_call(
        functools.partial(attn_kernel, pairs=pairs), grid=(lat, chan // width), in_specs=[qs, qs, qs, vs, vs], out_specs=qs,
        out_shape=like(q.shape), compiler_params=params(60),
        cost_estimate=cost(8 * lat * tok * tok * chan, 12 * lat * tok * chan), name="attn")(q, k0, k1, v0, v1)


def context_kernel(ctx_ref, w_ref, k_ref, v_ref):
    lat, padded, depth = ctx_ref.shape
    tokens = ctx_ref[...].reshape(lat * padded, depth)
    keys = dot_nt(tokens, w_ref[0, 0]).astype(BF)
    values = dot_nt(w_ref[0, 1], tokens).astype(BF)
    for l in range(lat):
        k_ref[0, l] = keys[l * padded:l * padded + CTX_ROWS]
        v_ref[0, l] = values[:, at_lanes(l, padded)]


def context_call(ctx, ckv_t):
    lat, padded, depth = ctx.shape
    layers, _, chan, _ = ckv_t.shape
    return pl.pallas_call(
        context_kernel, grid=(layers,),
        in_specs=[whole(ctx), major((1, 2, chan, depth))],
        out_specs=[major((1, lat, CTX_ROWS, chan)), major((1, lat, chan, padded))],
        out_shape=[like((layers, lat, CTX_ROWS, chan)), like((layers, lat, chan, padded))],
        compiler_params=params(60), cost_estimate=cost(4 * layers * lat * padded * depth * chan, 4 * layers * depth * chan), name="context")(ctx, ckv_t)


def cross_attend(q_s, kc_ref, vc_ref, o_s, ctx_len):
    tok, chan = q_s.shape

    def scores(p):
        kc = kc_ref[0, 0, :, at_lanes(p)]
        lane = lax.broadcasted_iota(jnp.int32, kc.shape, 1)
        zero = jnp.zeros_like(kc)
        both = jnp.concatenate([jnp.where(lane < HEAD, kc, zero), jnp.where(lane >= HEAD, kc, zero)], axis=0)
        return dot_nt(both, q_s[:, at_lanes(p)])

    pairs = chan // LANES
    coming = scores(0)
    for p in range(pairs):
        s = coming
        if p + 1 < pairs:
            coming = scores(p + 1)
        exps, sums = [], []
        for h in range(2):
            sh = s[at_lanes(h, CTX_ROWS)]
            valid = lax.broadcasted_iota(jnp.int32, sh.shape, 0) < ctx_len
            sh = jnp.where(valid, sh, -jnp.inf)
            e = jnp.exp2((sh - col_max(sh)) * SOFTMAX_MUL)
            sums.append(col_sum(e))
            exps += [e.astype(BF), jnp.zeros((LANES - CTX_ROWS, tok), BF)]
        vc = vc_ref[0, 0, at_lanes(p), :]
        row = lax.broadcasted_iota(jnp.int32, vc.shape, 0)
        zero = jnp.zeros_like(vc)
        vb = jnp.concatenate([jnp.where(row < HEAD, vc, zero), jnp.where(row >= HEAD, vc, zero)], axis=1)
        o = dot(vb, jnp.concatenate(exps, axis=0))
        o = jnp.concatenate([o[:HEAD] / sums[0], o[HEAD:] / sums[1]], axis=0)
        o_s[:, at_lanes(p)] = jnp.transpose(o).astype(BF)


def rest_kernel(att_ref, u_ref, wo_ref, ab_ref, ln_ref, wq_ref, kc_ref, vc_ref, wc_ref, w1a_ref, w1b_ref, b1a_ref, b1b_ref, w2_ref, b2_ref, out_ref, q_s, o_s, u_s, n_s, acc_s, *, layer, ctx_len, lat, chunk):
    step = pl.program_id(0)
    tok = u_ref.shape[1]
    chunks = [at_lanes(i, tok // CHUNKS) for i in range(CHUNKS)]

    @pl.when(step < lat)
    def _():
        for rr in chunks:
            u_s[rr] = (dot(att_ref[0, rr], wo_ref[0, 0]) + u_ref[0, rr].astype(F32) + row_of(ab_ref, layer, 0)).astype(BF)
        for rr in chunks:
            q_s[rr] = dot_nt(layer_norm(u_s[rr].astype(F32), *affine(ln_ref, layer, 1)), wq_ref[0]).astype(BF)
        cross_attend(q_s, kc_ref, vc_ref, o_s, ctx_len)
        for rr in chunks:
            y = (dot(o_s[rr], wc_ref[0, 0]) + u_s[rr].astype(F32) + row_of(ab_ref, layer, 1)).astype(BF).astype(F32)
            rows = pl.ds(pl.multiple_of(step * tok + rr.start, LANES), rr.stop - rr.start)
            n_s[rows] = layer_norm(y, *affine(ln_ref, layer, 2))
            acc_s[rows] = y + row_of(b2_ref, layer)

    @pl.when(step >= lat)
    def _():
        for m in range(n_s.shape[0] // chunk):
            rr = at_lanes(m, chunk)
            n = n_s[rr]
            p2 = dot(n, w1b_ref[0]) + row_of(b1b_ref, layer)
            p1 = dot(n, w1a_ref[0]) + row_of(b1a_ref, layer)
            half = 0.5 * p2
            gated = (p1 * (half + half * lax.erf(p2 * math.sqrt(0.5)))).astype(BF)
            acc_s[rr] += dot(gated, w2_ref[0])

    @pl.when(step == pl.num_programs(0) - 1)
    def _():
        out_ref[...] = acc_s[...].astype(BF)


def rest_call(att, u, attn_out, attn_b, ln_par, cq_t, kc, vc, w1, b1, w2, b2, layer, ctx_len, ft=512, chunk=512):
    lat, tok, chan = u.shape
    width = w2.shape[1]
    n = width // ft
    row = pl.BlockSpec((1, tok, chan), lambda i: (jnp.minimum(i, lat - 1), 0, 0))
    ctx_spec = lambda a: pl.BlockSpec((1, 1) + a.shape[2:], lambda i: (layer, jnp.minimum(i, lat - 1), 0, 0))
    mat = lambda i: fixed((1, 1, chan, chan), layer, i)
    part = lambda i: jnp.maximum(i - lat, 0)
    flat = (lat * tok, chan)
    return pl.pallas_call(
        functools.partial(rest_kernel, layer=layer, ctx_len=ctx_len, lat=lat, chunk=chunk), grid=(lat + n,),
        in_specs=[row, row, mat(0), whole(attn_b), whole(ln_par), fixed((1, chan, chan), layer), ctx_spec(kc), ctx_spec(vc), mat(1),
                  pl.BlockSpec((1, chan, ft), lambda i: (layer, 0, part(i))), pl.BlockSpec((1, chan, ft), lambda i: (layer, 0, part(i) + n)),
                  pl.BlockSpec((w1.shape[0], ft), lambda i: (0, part(i))), pl.BlockSpec((w1.shape[0], ft), lambda i: (0, part(i) + n)),
                  pl.BlockSpec((1, ft, chan), lambda i: (layer, part(i), 0)), whole(b2)],
        out_specs=fixed(flat), out_shape=like(flat),
        scratch_shapes=[pltpu.VMEM((tok, chan), BF)] * 3 + [pltpu.VMEM(flat, BF), pltpu.VMEM(flat, F32)],
        compiler_params=params(62), cost_estimate=cost(6 * lat * tok * chan * (chan + width), 6 * chan * (chan + width)), name="rest")(
            att, u, attn_out, attn_b, ln_par, cq_t, kc, vc, attn_out, w1, w1, b1, b1, w2, b2)


def leave_kernel(core_ref, u_ref, w_ref, pb_ref, h_ref, out_ref, sum_ref, edge_ref):
    sums, squares = [], []
    core = core_ref[0]
    tok = u_ref.shape[1]
    for l in range(u_ref.shape[0]):
        y = dot(u_ref[l], w_ref[0]) + row_of(pb_ref, 1) + h_ref[l].astype(F32)
        y = y.astype(BF)
        out_ref[l] = y
        edge_ref[l] = jnp.where(core == 0, y[tok - LANES:], y[:LANES])
        y = y.astype(F32)
        sums.append(col_sum(y))
        squares.append(col_sum(y * y))
    sum_ref[...] = place_rows(sums, squares, 0)


def leave_call(core, u, proj_w, proj_b, h, nt=256):
    lat, tok, chan = u.shape
    return pl.pallas_call(
        leave_kernel,
        grid_spec=pltpu.PrefetchScalarGridSpec(
            num_scalar_prefetch=1, grid=(chan // nt,),
            in_specs=[whole(u), minor((1, chan, nt), 1), minor((2, nt)), minor((lat, tok, nt))],
            out_specs=[minor((lat, tok, nt)), minor((SUM_ROWS, nt)), minor((lat, LANES, nt))]),
        out_shape=[like(u.shape), like((SUM_ROWS, chan), F32), like((lat, LANES, chan))],
        compiler_params=params(60), cost_estimate=cost(2 * lat * tok * chan * chan, 2 * chan * chan), name="leave")(core, u, proj_w, proj_b, h)


SWAP = pairs_of('01 10 23 32')


def device_block(latents, time_emb, context, res_norm, res_conv_w, res_conv_b, res_temb_w, res_temb_b, tr_norm, proj_w, proj_b, ln_par, self_qkv, cross_q, cross_kv, attn_out, attn_b, ff_in_w, ff_in_b, ff_out_w, ff_out_b):
    index = lax.axis_index('sp')
    chip, core = index // 2, index % 2
    core_vec = jnp.reshape(core, (1,)).astype(jnp.int32)
    count, rows_n, cols, chan = latents.shape
    lat = count // 2
    tok = 2 * rows_n * cols
    ctx_len = context.shape[1]
    where = jnp.reshape(index, (1,)).astype(jnp.int32)
    flat = latents.reshape(count, rows_n * cols, chan)
    halves = flat.reshape(2, lat, rows_n * cols, chan)
    going, staying = lax.dynamic_index_in_dim(halves, 1 - core, keepdims=False), lax.dynamic_index_in_dim(halves, core, keepdims=False)

    def spread(away, here):
        return lax.ppermute(away, 'sp', pairs_of('02 10 23 31')), lax.ppermute(here, 'sp', pairs_of('12 21 00 33'))

    early = spread(going[lat - 1:], staying[lat - 1:])
    *rest, context = lax.optimization_barrier((going[:lat - 1], staying[:lat - 1], context))
    late = spread(*rest)

    temb = lax.dynamic_slice(time_emb, (chip * lat, 0), (lat, chan))
    temb = jax.nn.silu(temb.astype(F32)).astype(BF)
    tembs = [dot(temb, res_temb_w[r]) + res_temb_b[r] for r in range(2)]
    ctx = lax.dynamic_slice(context, (chip * lat, 0, 0), (lat,) + context.shape[1:])
    ctx = jnp.pad(ctx, ((0, 0), (0, LANES - ctx_len), (0, 0)))
    ckv_t = jnp.moveaxis(cross_kv, 2, -1).reshape(cross_kv.shape[:2] + (chan, -1))
    kc, vc = context_call(ctx, ckv_t)
    qkv_t = jnp.moveaxis(self_qkv, 2, -1).reshape(self_qkv.shape[:2] + (chan, chan))
    cq_t = jnp.moveaxis(cross_q, 1, -1).reshape(-1, chan, chan)
    attn_w = attn_out.reshape(attn_b.shape[:2] + (chan, chan))
    conv_w = res_conv_w.reshape(-1, KERNEL, KERNEL * chan, chan)

    swap = lambda a: lax.ppermute(a, 'sp', SWAP)
    early, kc, vc, tembs[0] = lax.optimization_barrier((early, kc, vc, tembs[0]))
    v, own, edge = gather_call(where, *early, 2)
    into = conv_call(where, v, swap(edge), own, swap(own), res_norm, res_conv_b, conv_w, 0, 0, temb=tembs[0], base=2, lat=1)
    late, v, into, tembs[1] = lax.optimization_barrier((late, v, into, tembs[1]))
    v, own, edge = gather_call(where, *late, 0, into=v)
    t, sums_t, edge = conv_call(where, v, swap(edge), own, swap(own), res_norm, res_conv_b, conv_w, 0, 0, temb=tembs[0], into=into, base=0, lat=2)
    h, sums_h, _ = conv_call(where, t, swap(edge), sums_t, swap(sums_t), res_norm, res_conv_b, conv_w, 0, 1, res=v)
    u, n, k = enter_call(h, sums_h, swap(sums_h), tr_norm, proj_w, proj_b, ln_par, qkv_t)
    for layer in range(2):
        if layer:
            n, k = key_call(u, ln_par, qkv_t, layer)
        k_far = swap(k)
        vals = linear_call(value_kernel, n, qkv_t, layer, 2, (chan, tok), "values")
        vals_far = swap(vals)
        q = linear_call(query_kernel, n, qkv_t, layer, 0, (tok, chan), "queries")
        att = attn_call(q, k, k_far, vals, vals_far)
        u = rest_call(att, u, attn_w, attn_b, ln_par, cq_t, kc, vc, ff_in_w, ff_in_b, ff_out_w, ff_out_b, layer, ctx_len).reshape(lat, tok, chan)
    h, sums_h, edge = leave_call(core_vec, u, proj_w, proj_b, h)
    t, sums_t, edge = conv_call(where, h, swap(edge), sums_h, swap(sums_h), res_norm, res_conv_b, conv_w, 1, 0, temb=tembs[1])
    edge, peer = swap(edge), swap(sums_t)
    lows, highs = [], []
    for base, some in ((0, 2), (2, 1)):
        going, staying = conv_call(where, t, edge, sums_t, peer, res_norm, res_conv_b, conv_w, 1, 1, res=h, base=base, lat=some, want_sums=False)
        first = lax.ppermute(going, 'sp', pairs_of('20 01 32 13'))
        third = lax.ppermute(staying, 'sp', pairs_of('21 12 00 33'))
        lows.append(jnp.where(core == 0, third, first))
        highs.append(jnp.where(core == 0, first, third))
    return jnp.concatenate(lows + highs, axis=0).reshape(latents.shape)


def solution(mesh):
    row_spec = P('dp', 'sp')
    part_spec = P('dp')
    in_specs = (row_spec, part_spec, part_spec) + (P(),) * 18
    return jax.shard_map(device_block, mesh=mesh, in_specs=in_specs, out_specs=row_spec, check_vma=False)
```
